8 devices in a mesh: dp: 1 (over z), tp: 8 (over x, y, core).
Axes of the slice: x: 2, y: 2, z: 1, core: 2. Of those that a mesh axis runs over, the one named last changes fastest.
Arguments:
- x: bfloat16 [4096, 2048], P(('dp', 'tp'))
- gain: bfloat16 [2048], replicated
- wq: bfloat16 [2048, 3072], P(None, 'tp')
- wk: bfloat16 [2048, 3072], P(None, 'tp')
- wv: bfloat16 [2048, 3072], P(None, 'tp')
- wo: bfloat16 [3072, 2048], P('tp')
Outputs:
- output: bfloat16 [4096, 2048], P(('dp', 'tp'))
All inputs are finite; a program needn't handle non-finite values.
Results may differ from the reference program's by a relative error of at most 0.012.
Values are sent between devices in bfloat16 or wider.
A program may use at most 2 GiB of HBM per device.

```python
import jax
import jax.numpy as jnp
from jax import lax

ROWS = 4096
D = 2048
HEADS = 24
KV_HEADS = 24
HEAD = 128
THETA = 10000


def setup_inputs(seed: int = 0, part: int = 0) -> dict:
    kx, kn, kq, kk, kv, ko = jax.random.split(jax.random.key(seed), 6)

    def weights(key, rows, columns):
        return jax.random.normal(key, (rows, columns), jnp.float32) * rows**-0.5

    drawn = {
        "x": jax.random.normal(jax.random.fold_in(kx, part), (ROWS, D), jnp.float32),
        "gain": 1 + 0.1 * jax.random.normal(kn, (D,), jnp.float32),
        "wq": 2 * weights(kq, D, HEADS * HEAD),
        "wk": 2 * weights(kk, D, KV_HEADS * HEAD),
        "wv": 4 * weights(kv, D, KV_HEADS * HEAD),
        "wo": weights(ko, HEADS * HEAD, D),
    }
    return {k: v.astype(jnp.bfloat16) for k, v in drawn.items()}


def normed(x, gain):
    wide = x.astype(jnp.float32)
    scale = lax.rsqrt(jnp.mean(wide * wide, -1, keepdims=True) + 1e-6)
    return (wide * scale * gain.astype(jnp.float32)).astype(jnp.bfloat16)


def turned(t, place, theta):
    half = t.shape[-1] // 2
    angle = place.astype(jnp.float32)[:, None] * theta ** (-jnp.arange(half, dtype=jnp.float32) / half)
    cos, sin = jnp.cos(angle)[:, None], jnp.sin(angle)[:, None]
    a, b = t[..., :half].astype(jnp.float32), t[..., half:].astype(jnp.float32)
    return jnp.concatenate([a * cos - b * sin, b * cos + a * sin], -1).astype(jnp.bfloat16)


def matmul(a, w):
    return jnp.dot(a, w, preferred_element_type=jnp.float32).astype(jnp.bfloat16)


def einsum(form, a, b):
    return jnp.einsum(form, a.astype(jnp.float32), b.astype(jnp.float32))


def attention(q, k, v):
    scores = einsum("tgsd,ugd->gstu", q, k) * q.shape[-1] ** -0.5
    token = jnp.arange(q.shape[0])
    scores = jnp.where(token[:, None] >= token, scores, -jnp.inf)
    weights = jax.nn.softmax(scores, -1).astype(jnp.bfloat16)
    return einsum("gstu,ugd->tgsd", weights, v).astype(jnp.bfloat16)


def reference(x, gain, wq, wk, wv, wo):
    a, place = normed(x, gain), jnp.arange(ROWS)
    q = turned(matmul(a, wq).reshape(ROWS, HEADS, HEAD), place, THETA).reshape(ROWS, KV_HEADS, -1, HEAD)
    k = turned(matmul(a, wk).reshape(ROWS, KV_HEADS, HEAD), place, THETA)
    v = matmul(a, wv).reshape(ROWS, KV_HEADS, HEAD)
    seen = attention(q, k, v).reshape(ROWS, HEADS * HEAD)
    return (x.astype(jnp.float32) + jnp.dot(seen, wo, preferred_element_type=jnp.float32)).astype(jnp.bfloat16)
```

```python
import functools

import jax
import jax.numpy as jnp
import numpy as np
from jax import lax
from jax.experimental import pallas as pl
from jax.experimental.pallas import tpu as pltpu
from jax.sharding import PartitionSpec as P

MESH = pl.DeviceIdType.MESH
NEG = -1e30
HIDDEN = 2 * NEG
LOG2E = 1.4426950408889634
HEAD = 128
THETA = 10000
N = 3
BLK = 256
ROWS = 512
NBLK = 16
D = 2048
W = N * HEAD
VR = 144


def _dot(a, b, ca, cb):
    return lax.dot_general(a, b, (((ca,), (cb,)), ((), ())), preferred_element_type=jnp.float32)


def _rope_tables():
    half = HEAD // 2
    freq = THETA ** (-np.arange(half, dtype=np.float64) / half)
    sign = np.concatenate([-np.ones(half), np.ones(half)])
    def table(pos):
        ang = pos[:, None] * np.concatenate([freq, freq])
        return np.cos(ang).astype(np.float32), (np.sin(ang) * sign).astype(np.float32)
    lo = np.stack(table(np.arange(BLK, dtype=np.float64)))
    hi = np.stack(table(np.arange(NBLK, dtype=np.float64) * BLK))
    return lo, hi


def _place(me):
    core = me % 2
    y = (me // 2) % 2
    x = me // 4
    base = me - core
    xn = base + 4 - 8 * x
    yn = base + 2 - 4 * y
    dg = xn + 2 - 4 * y
    return core, base, xn, yn, dg


def _block(me, k, side):
    core, base, xn, yn, dg = _place(me)
    odd = k % 2
    flip = side + odd - 2 * side * odd
    near = jnp.where(side == 0, xn, yn) if not isinstance(side, int) else (xn if side == 0 else yn)
    dev = jnp.where(k < 1, me, jnp.where(k < 2, me + 1 - 2 * core, jnp.where(k < 6, near + flip, dg + 1 - flip)))
    half = jnp.where((k == 2) | (k == 3), 1 - side, side)
    return 2 * dev + half


def kernel_a(x_ref, gain_ref, wq_ref, wk_ref, wv_ref, lo_ref, hi_ref, o_ref,
             a_s, w_s, q_s, k_s, v_s, top_s, mix_s, wsem, send, recv):
    me = lax.axis_index("tp")
    core, base, xn, yn, dg = _place(me)
    partner = base + 1 - core
    link = jnp.where(core == 0, xn, yn + 1)
    first = 1 - core

    loads = [pltpu.make_async_copy(w, w_s.at[:, pl.ds(i * W, W)], wsem.at[i]) for i, w in enumerate((wq_ref, wk_ref, wv_ref))]
    for c in loads:
        c.start()

    barrier = pltpu.get_barrier_semaphore()
    for other in (partner, link):
        pl.semaphore_signal(barrier, inc=1, device_id={"tp": other}, device_id_type=MESH)

    def slot(s):
        return a_s.at[pl.ds(pl.multiple_of(s * BLK, BLK), BLK), :]

    def remote(src, dst, sem, dev):
        return pltpu.make_async_remote_copy(src_ref=slot(src), dst_ref=slot(dst), send_sem=send.at[sem], recv_sem=recv.at[dst],
                                            device_id={"tp": dev}, device_id_type=MESH)

    def arrived(s):
        return pltpu.make_async_remote_copy(src_ref=slot(s), dst_ref=slot(s), send_sem=send.at[0], recv_sem=recv.at[s],
                                            device_id={"tp": partner}, device_id_type=MESH).wait_recv()

    gain = gain_ref[...].astype(jnp.float32)

    def norm(start, count):
        def rows(i, _):
            at = pl.ds(pl.multiple_of(start + i * 16, 16), 16)
            wide = x_ref[at, :].astype(jnp.float32)
            scale = lax.rsqrt(jnp.mean(wide * wide, -1, keepdims=True) + 1e-6)
            a_s[at, :] = (wide * scale * gain).astype(jnp.bfloat16)
        lax.fori_loop(0, count // 16, rows, None, unroll=2)

    norm(first * BLK, BLK)
    pl.semaphore_wait(barrier, 2)
    norm((1 - first) * BLK, BLK // 2)
    remote(first, 4 + core, 2, link).start()
    remote(first, 2 + first, 0, partner).start()
    norm((1 - first) * BLK + BLK // 2, BLK // 2)
    v_s[:, :, HEAD:, :] = jnp.ones((NBLK, N, VR - HEAD, BLK), jnp.bfloat16)
    top_s[...] = jnp.full(top_s.shape, NEG, jnp.float32)
    def clear(i, _):
        mix_s[i] = jnp.zeros(mix_s.shape[1:], jnp.float32)
    lax.fori_loop(0, NBLK, clear, None)
    remote(1 - first, 3 - first, 1, partner).start()
    for c in loads:
        c.wait()

    scale_e = HEAD ** -0.5 * LOG2E

    def project(k, blocks):
        here = pl.ds(pl.multiple_of(k * ROWS, ROWS), ROWS)
        tables = []
        for b in blocks:
            ch, sh = hi_ref[0, pl.ds(b, 1), :], hi_ref[1, pl.ds(b, 1), :]
            cl, sl = lo_ref[0], lo_ref[1]
            tables.append((ch * cl - sh * sl, sh * cl + ch * sl))
        for g in range(0, 3 * N, 2):
            width = min(2, 3 * N - g) * HEAD
            out = _dot(a_s[here, :], w_s[:, g * HEAD : g * HEAD + width], 1, 0).astype(jnp.bfloat16)
            for i in range(width // HEAD):
                kind, n = divmod(g + i, N)
                for b, block in enumerate(blocks):
                    t = out[b * BLK : (b + 1) * BLK, i * HEAD : (i + 1) * HEAD]
                    if kind == 2:
                        v_s[block, n, :HEAD, :] = t.T
                    else:
                        t = t.astype(jnp.float32)
                        t = t * tables[b][0] + pltpu.roll(t, HEAD // 2, 1) * tables[b][1]
                        (q_s if kind == 0 else k_s)[block, n] = t.astype(jnp.bfloat16)

    def attend(pairs):
        strips = [(q, k, masked, n) for q, k, masked in pairs for n in range(N)]
        scores = [_dot(k_s[k, n], q_s[q, n], 1, 1) for q, k, _, n in strips]
        if any(masked for _, _, masked in pairs):
            ok = lax.broadcasted_iota(jnp.int32, (BLK, BLK), 1) >= lax.broadcasted_iota(jnp.int32, (BLK, BLK), 0)
        for (q, k, masked, n), s in zip(strips, scores):
            if masked:
                s = jnp.where(ok, s, HIDDEN)
            old = top_s[q, n : n + 1, :]
            top = jnp.maximum(old, s.max(axis=0, keepdims=True))
            top_s[q, n : n + 1, :] = top
            p = jnp.exp2((s - top) * scale_e).astype(jnp.bfloat16)
            keep = jnp.exp2((old - top) * scale_e)
            mix_s[q, n] = mix_s[q, n] * keep + _dot(v_s[k, n], p, 1, 0)[: HEAD + 8, :]

    def event(k, _):
        b0, b1 = _block(me, k, 0), _block(me, k, 1)

        @pl.when(k >= 2)
        def _():
            arrived(2 * k + 1 - core)

            @pl.when(k < 4)
            def _():
                remote(2 * k + 1 - core, 2 * k + 8 + core, 4 + k, link).start()

        project(k, (b0, b1))

        @pl.when(k == 0)
        def _():
            arrived(2 + first)
            remote(2 + first, 6 + core, 3, link).start()
            remote(1 - first, 8 + core, 4, link).start()
            arrived(3 - first)
            remote(3 - first, 10 + core, 5, link).start()

        def older(j, _):
            pairs = []
            for new in (b0, b1):
                for side in (0, 1):
                    b = _block(me, j, side)
                    pairs.append((jnp.maximum(new, b), jnp.minimum(new, b), False))
            attend(pairs)

        lax.fori_loop(0, k, older, None)

        @pl.when((k >= 1) & (k < 7))
        def _():
            arrived(2 * k + 2 + core)
            remote(2 * k + 2 + core, 2 * k + 2 + core, 7 + k, partner).start()

        attend([(jnp.maximum(b0, b1), jnp.minimum(b0, b1), False), (b0, b0, True), (b1, b1, True)])

    lax.fori_loop(0, 8, event, None)

    def finish(b, _):
        for n in range(N):
            out = mix_s[b, n, :HEAD, :] * (1 / mix_s[b, n, HEAD : HEAD + 1, :])
            o_ref[pl.ds(pl.multiple_of(b * BLK, BLK), BLK), n * HEAD : (n + 1) * HEAD] = out.astype(jnp.bfloat16).T
    lax.fori_loop(0, NBLK, finish, None)

    for i in range(14):
        remote(0, 0, i, partner).wait_send()


def attended(x, gain, wq, wk, wv):
    lo, hi = _rope_tables()
    any_space = pl.BlockSpec(memory_space=pl.ANY)
    vmem = pl.BlockSpec(memory_space=pltpu.VMEM)
    return pl.pallas_call(
        kernel_a,
        out_shape=jax.ShapeDtypeStruct((8 * ROWS, W), jnp.bfloat16),
        in_specs=[vmem, vmem, any_space, any_space, any_space, vmem, vmem],
        out_specs=vmem,
        scratch_shapes=[
            pltpu.VMEM((NBLK * BLK, D), jnp.bfloat16),
            pltpu.VMEM((D, 3 * W), jnp.bfloat16),
            pltpu.VMEM((NBLK, N, BLK, HEAD), jnp.bfloat16),
            pltpu.VMEM((NBLK, N, BLK, HEAD), jnp.bfloat16),
            pltpu.VMEM((NBLK, N, VR, BLK), jnp.bfloat16),
            pltpu.VMEM((NBLK, 8, BLK), jnp.float32),
            pltpu.VMEM((NBLK, N, HEAD + 8, BLK), jnp.float32),
            pltpu.SemaphoreType.DMA((3,)),
            pltpu.SemaphoreType.DMA((14,)),
            pltpu.SemaphoreType.DMA((16,)),
        ],
        compiler_params=pltpu.CompilerParams(collective_id=0, has_side_effects=True, vmem_limit_bytes=63 * 2**20),
        cost_estimate=pl.CostEstimate(flops=40 * 10**9, bytes_accessed=10**7, transcendentals=3 * 10**7),
    )(x, gain.reshape(1, -1), wq, wk, wv, jnp.asarray(lo), jnp.asarray(hi))


def solution(mesh):
    def step(x, gain, wq, wk, wv, wo):
        seen = attended(x, gain, wq, wk, wv)
        term = jnp.dot(seen, wo, preferred_element_type=jnp.float32)
        y = lax.psum_scatter(term.astype(jnp.bfloat16), "tp", scatter_dimension=0, tiled=True)
        return (x.astype(jnp.float32) + y.astype(jnp.float32)).astype(jnp.bfloat16)

    tokens, columns = P(("dp", "tp"), None), P(None, "tp")
    return jax.shard_map(
        step,
        mesh=mesh,
        in_specs=(tokens, P(None), columns, columns, columns, P("tp", None)),
        out_specs=tokens,
        check_vma=False,
    )
```

```python
import functools

import jax
import jax.numpy as jnp
import numpy as np
from jax import lax
from jax.experimental import pallas as pl
from jax.experimental.pallas import tpu as pltpu
from jax.sharding import PartitionSpec as P

MESH = pl.DeviceIdType.MESH
NEG = -1e30
HIDDEN = 2 * NEG
LOG2E = 1.4426950408889634
HEAD = 128
THETA = 10000
N = 3
BLK = 256
ROWS = 512
NBLK = 16
D = 2048
W = N * HEAD
VR = 144
MR = HEAD + 8


def _dot(a, b, ca, cb):
    return lax.dot_general(a, b, (((ca,), (cb,)), ((), ())), preferred_element_type=jnp.float32)


def _rope_tables():
    half = HEAD // 2
    freq = THETA ** (-np.arange(half, dtype=np.float64) / half)
    sign = np.concatenate([-np.ones(half), np.ones(half)])
    def table(pos):
        ang = pos[:, None] * np.concatenate([freq, freq])
        return np.cos(ang).astype(np.float32), (np.sin(ang) * sign).astype(np.float32)
    lo = np.stack(table(np.arange(BLK, dtype=np.float64)))
    hi = np.stack(table(np.arange(NBLK, dtype=np.float64) * BLK))
    return lo, hi


def _place(me):
    core = me % 2
    y = (me // 2) % 2
    x = me // 4
    base = me - core
    xn = base + 4 - 8 * x
    yn = base + 2 - 4 * y
    dg = xn + 2 - 4 * y
    return core, base, xn, yn, dg


def _block(me, k, side):
    core, base, xn, yn, dg = _place(me)
    odd = k % 2
    flip = side + odd - 2 * side * odd
    near = jnp.where(side == 0, xn, yn) if not isinstance(side, int) else (xn if side == 0 else yn)
    dev = jnp.where(k < 1, me, jnp.where(k < 2, me + 1 - 2 * core, jnp.where(k < 6, near + flip, dg + 1 - flip)))
    half = jnp.where((k == 2) | (k == 3), 1 - side, side)
    return 2 * dev + half


def kernel(x_ref, gain_ref, wq_ref, wk_ref, wv_ref, wo_ref, lo_ref, hi_ref, y_ref,
           a_s, w_s, q_s, k_s, v_s, top_s, mix_s, wo_s, seen_s, part_s, sum_s, wsem, send, recv, send2, recv2, lsem):
    me = lax.axis_index("tp")
    core, base, xn, yn, dg = _place(me)
    partner = base + 1 - core
    link = jnp.where(core == 0, xn, yn + 1)
    first = 1 - core

    loads = [pltpu.make_async_copy(w, w_s.at[:, pl.ds(i * W, W)], wsem.at[i]) for i, w in enumerate((wq_ref, wk_ref, wv_ref))]
    for c in loads:
        c.start()
    wo_mine = wo_s.at[pl.ds(pl.multiple_of((2 + core) * W, W), W), :]
    wo_load = pltpu.make_async_copy(wo_ref, wo_mine, wsem.at[3])
    wo_load.start()

    barrier = pltpu.get_barrier_semaphore()
    for other in (partner, xn, xn + 1, yn, yn + 1):
        pl.semaphore_signal(barrier, inc=1, device_id={"tp": other}, device_id_type=MESH)

    def slot(s):
        return a_s.at[pl.ds(pl.multiple_of(s * BLK, BLK), BLK), :]

    def remote(src, dst, sem, dev):
        return pltpu.make_async_remote_copy(src_ref=slot(src), dst_ref=slot(dst), send_sem=send.at[sem], recv_sem=recv.at[dst],
                                            device_id={"tp": dev}, device_id_type=MESH)

    def send_wo(src, dst, sem, dev):
        at = lambda i: wo_s.at[pl.ds(pl.multiple_of(i * W, W), W), :]
        return pltpu.make_async_remote_copy(src_ref=at(src), dst_ref=at(dst), send_sem=send2.at[sem], recv_sem=recv2.at[dst],
                                            device_id={"tp": dev}, device_id_type=MESH)

    def arrived(s):
        return pltpu.make_async_remote_copy(src_ref=slot(s), dst_ref=slot(s), send_sem=send.at[0], recv_sem=recv.at[s],
                                            device_id={"tp": partner}, device_id_type=MESH).wait_recv()

    def wo_arrived(i):
        send_wo(i, i, 0, partner).wait_recv()

    gain = gain_ref[...].astype(jnp.float32)

    def norm(start, count):
        def rows(i, _):
            at = pl.ds(pl.multiple_of(start + i * 16, 16), 16)
            wide = x_ref[at, :].astype(jnp.float32)
            scale = lax.rsqrt(jnp.mean(wide * wide, -1, keepdims=True) + 1e-6)
            a_s[at, :] = (wide * scale * gain).astype(jnp.bfloat16)
        lax.fori_loop(0, count // 16, rows, None, unroll=2)

    norm(first * BLK, BLK)
    pl.semaphore_wait(barrier, 5)
    norm((1 - first) * BLK, BLK // 2)
    remote(first, 4 + core, 2, link).start()
    remote(first, 2 + first, 0, partner).start()
    norm((1 - first) * BLK + BLK // 2, BLK // 2)
    v_s[:, :, HEAD:, :] = jnp.ones((NBLK, N, VR - HEAD, BLK), jnp.bfloat16)
    top_s[...] = jnp.full(top_s.shape, NEG, jnp.float32)

    def clear(i, _):
        mix_s[pl.ds(pl.multiple_of(i * MR, MR), MR), :] = jnp.zeros((MR, BLK), jnp.float32)

    lax.fori_loop(0, NBLK * N, clear, None)
    remote(1 - first, 3 - first, 1, partner).start()
    for c in loads:
        c.wait()
    wo_load.wait()
    send_wo(2 + core, 2 + core, 0, partner).start()

    scale_e = HEAD ** -0.5 * LOG2E

    def project(k, blocks):
        here = pl.ds(pl.multiple_of(k * ROWS, ROWS), ROWS)
        tables = []
        for b in blocks:
            ch, sh = hi_ref[0, pl.ds(b, 1), :], hi_ref[1, pl.ds(b, 1), :]
            cl, sl = lo_ref[0], lo_ref[1]
            tables.append((ch * cl - sh * sl, sh * cl + ch * sl))
        for g in range(0, 3 * N, 2):
            width = min(2, 3 * N - g) * HEAD
            out = _dot(a_s[here, :], w_s[:, g * HEAD : g * HEAD + width], 1, 0).astype(jnp.bfloat16)
            for i in range(width // HEAD):
                kind, n = divmod(g + i, N)
                for b, block in enumerate(blocks):
                    t = out[b * BLK : (b + 1) * BLK, i * HEAD : (i + 1) * HEAD]
                    if kind == 2:
                        v_s[block, n, :HEAD, :] = t.T
                    else:
                        t = t.astype(jnp.float32)
                        t = t * tables[b][0] + pltpu.roll(t, HEAD // 2, 1) * tables[b][1]
                        (q_s if kind == 0 else k_s)[block, n] = t.astype(jnp.bfloat16)

    def attend(pairs):
        strips = [(q, k, masked, n) for q, k, masked in pairs for n in range(N)]
        scores = [_dot(k_s[k, n], q_s[q, n], 1, 1) for q, k, _, n in strips]
        if any(masked for _, _, masked in pairs):
            ok = lax.broadcasted_iota(jnp.int32, (BLK, BLK), 1) >= lax.broadcasted_iota(jnp.int32, (BLK, BLK), 0)
        for (q, k, masked, n), s in zip(strips, scores):
            if masked:
                s = jnp.where(ok, s, HIDDEN)
            old = top_s[q, n : n + 1, :]
            top = jnp.maximum(old, s.max(axis=0, keepdims=True))
            top_s[q, n : n + 1, :] = top
            p = jnp.exp2((s - top) * scale_e).astype(jnp.bfloat16)
            keep = jnp.exp2((old - top) * scale_e)
            mix = pl.ds(pl.multiple_of((q * N + n) * MR, 8), MR)
            mix_s[mix, :] = mix_s[mix, :] * keep + _dot(v_s[k, n], p, 1, 0)[:MR, :]

    def event(k, _):
        b0, b1 = _block(me, k, 0), _block(me, k, 1)

        @pl.when(k >= 2)
        def _():
            arrived(2 * k + 1 - core)

            @pl.when(k < 4)
            def _():
                remote(2 * k + 1 - core, 2 * k + 8 + core, 4 + k, link).start()

            @pl.when(k == 3)
            def _():
                wo_arrived(3 - core)
                send_wo(2 + core, 5 * core, 1, link).start()
                send_wo(3 - core, 1 + 3 * core, 2, link).start()

        project(k, (b0, b1))

        @pl.when(k == 0)
        def _():
            arrived(2 + first)
            remote(2 + first, 6 + core, 3, link).start()
            remote(1 - first, 8 + core, 4, link).start()
            arrived(3 - first)
            remote(3 - first, 10 + core, 5, link).start()

        def older(j, _):
            pairs = []
            for new in (b0, b1):
                for side in (0, 1):
                    b = _block(me, j, side)
                    pairs.append((jnp.maximum(new, b), jnp.minimum(new, b), False))
            attend(pairs)

        lax.fori_loop(0, k, older, None)

        @pl.when((k >= 1) & (k < 7))
        def _():
            arrived(2 * k + 2 + core)
            remote(2 * k + 2 + core, 2 * k + 2 + core, 7 + k, partner).start()

        attend([(jnp.maximum(b0, b1), jnp.minimum(b0, b1), False), (b0, b0, True), (b1, b1, True)])

    lax.fori_loop(0, 8, event, None)

    def finish(b):
        rows = pl.ds(pl.multiple_of(b * BLK, BLK), BLK)
        for n in range(N):
            at = (b * N + n) * MR
            out = mix_s[pl.ds(pl.multiple_of(at, 8), HEAD), :] * (1 / mix_s[pl.ds(pl.multiple_of(at + HEAD, 8), 1), :])
            seen_s[rows, n * HEAD : (n + 1) * HEAD] = out.astype(jnp.bfloat16).T

    def seen(dev, half):
        return seen_s.at[pl.ds(pl.multiple_of((2 * dev + half) * BLK, BLK), BLK), :]

    def part(i, own, c):
        left = own == (i >= 2)
        return part_s.at[i, :, pl.ds(pl.multiple_of(c * W + (0 if left else 2 * W), HEAD), W)]

    def hand(src, i, own, sem, arrival, dev):
        return pltpu.make_async_remote_copy(src_ref=src, dst_ref=part(i, own, core), send_sem=send2.at[sem], recv_sem=recv2.at[arrival],
                                            device_id={"tp": dev}, device_id_type=MESH)

    for c in (0, 1):
        finish(2 * (dg + c))
        finish(2 * (dg + c) + 1)
        hand(seen(dg + c, 0), 0, False, 5 + c, 6 + core, xn + c).start()
        hand(seen(dg + c, 1), 2, False, 7 + c, 10 + core, yn + c).start()
    for c in (0, 1):
        finish(2 * (xn + c))
        hand(seen(xn + c, 0), 1, False, 9 + c, 8 + core, xn + c).start()
        finish(2 * (yn + c) + 1)
        hand(seen(yn + c, 1), 3, False, 11 + c, 12 + core, yn + c).start()
    for c in (0, 1):
        finish(2 * (yn + c))
        finish(2 * (xn + c) + 1)
        finish(2 * (base + c))
        finish(2 * (base + c) + 1)
    wanted = ((yn, 0), (base, 0), (xn, 1), (base, 1))
    for i, (chip, half) in enumerate(wanted):
        hand(seen(chip + 1 - core, half), i, True, 13 + i, 14 + i, partner).start()
    local = [pltpu.make_async_copy(seen(chip + core, half), part(i, True, core), lsem.at[i]) for i, (chip, half) in enumerate(wanted)]
    for c in local:
        c.start()

    for i in (0, 1):
        piece = 4 * core + (core + i - 2 * core * i)
        wo_arrived(piece)
        send_wo(piece, piece, 3 + i, partner).start()
    for i in (0, 1):
        wo_arrived(4 - 4 * core + i)
    for i in range(14):
        remote(0, 0, i, partner).wait_send()

    def ready(i):
        local[i].wait()
        hand(part(i, True, 0), i, True, 0, 14 + i, partner).wait_recv()
        for c in (0, 1):
            hand(part(i, True, 0), i, False, 0, 6 + 2 * i + c, partner).wait_recv()

    def product(i, rows, columns):
        return _dot(part_s[i, rows, :], wo_s[0 if i < 2 else 2 * W : 4 * W if i < 2 else 6 * W, columns], 1, 0)

    PIECE = 128

    def give(i, piece, dev):
        at = pl.ds(PIECE * (i + piece), PIECE)
        return pltpu.make_async_remote_copy(src_ref=a_s.at[at, :], dst_ref=sum_s.at[at, :], send_sem=send2.at[17 + i + piece],
                                            recv_sem=recv2.at[18 + i + piece], device_id={"tp": dev}, device_id_type=MESH)

    WIDE = 512
    for i, dev in ((0, yn + core), (2, xn + core)):
        ready(i)
        for piece in (0, 1):
            def columns(n, _):
                at = pl.ds(pl.multiple_of(n * WIDE, WIDE), WIDE)
                a_s[PIECE * (i + piece) : PIECE * (i + piece + 1), at] = product(i, slice(PIECE * piece, PIECE * (piece + 1)), at).astype(jnp.bfloat16)
            lax.fori_loop(0, D // WIDE, columns, None)
            give(i, piece, dev).start()
    for i in (1, 3):
        ready(i)

        def columns(n, _):
            out = product(i, slice(None), pl.ds(pl.multiple_of(n * BLK, BLK), BLK))
            mix_s[pl.ds(pl.multiple_of(n * ROWS + (i - 1) * PIECE, BLK), BLK), :] = out

        lax.fori_loop(0, D // BLK, columns, None)

    for piece in (0, 1):
        for i in (0, 2):
            give(i, piece, partner).wait_recv()
            r = PIECE * (i + piece)
            for n in range(D // BLK):
                at = slice(n * BLK, (n + 1) * BLK)
                total = mix_s[n * ROWS + r : n * ROWS + r + PIECE, :] + sum_s[r : r + PIECE, at].astype(jnp.float32)
                y_ref[r : r + PIECE, at] = (x_ref[r : r + PIECE, at].astype(jnp.float32) + total).astype(jnp.bfloat16)

    for i in range(5):
        send_wo(0, 0, i, partner).wait_send()
    for i in range(5, 17):
        hand(seen(0, 0), 0, True, i, 14, partner).wait_send()
    for i in (0, 2):
        for piece in (0, 1):
            give(i, piece, partner).wait_send()


def solution(mesh):
    def step(x, gain, wq, wk, wv, wo):
        lo, hi = _rope_tables()
        any_space = pl.BlockSpec(memory_space=pl.ANY)
        vmem = pl.BlockSpec(memory_space=pltpu.VMEM)
        return pl.pallas_call(
            kernel,
            out_shape=jax.ShapeDtypeStruct((ROWS, D), jnp.bfloat16),
            in_specs=[vmem, vmem, any_space, any_space, any_space, any_space, vmem, vmem],
            out_specs=vmem,
            scratch_shapes=[
                pltpu.VMEM((NBLK * BLK, D), jnp.bfloat16),
                pltpu.VMEM((D, 3 * W), jnp.bfloat16),
                pltpu.VMEM((NBLK, N, BLK, HEAD), jnp.bfloat16),
                pltpu.VMEM((NBLK, N, BLK, HEAD), jnp.bfloat16),
                pltpu.VMEM((NBLK, N, VR, BLK), jnp.bfloat16),
                pltpu.VMEM((NBLK, 8, BLK), jnp.float32),
                pltpu.VMEM((NBLK * N * MR, BLK), jnp.float32),
                pltpu.VMEM((6 * W, D), jnp.bfloat16),
                pltpu.VMEM((NBLK * BLK, W), jnp.bfloat16),
                pltpu.VMEM((4, BLK, 4 * W), jnp.bfloat16),
                pltpu.VMEM((ROWS, D), jnp.bfloat16),
                pltpu.SemaphoreType.DMA((4,)),
                pltpu.SemaphoreType.DMA((14,)),
                pltpu.SemaphoreType.DMA((16,)),
                pltpu.SemaphoreType.DMA((21,)),
                pltpu.SemaphoreType.DMA((22,)),
                pltpu.SemaphoreType.DMA((4,)),
            ],
            compiler_params=pltpu.CompilerParams(collective_id=0, has_side_effects=True, vmem_limit_bytes=67_043_328),
            cost_estimate=pl.CostEstimate(flops=40 * 10**9, bytes_accessed=10**7, transcendentals=3 * 10**7),
        )(x, gain.reshape(1, -1), wq, wk, wv, wo, jnp.asarray(lo), jnp.asarray(hi))

    tokens, columns = P(("dp", "tp"), None), P(None, "tp")
    return jax.shard_map(
        step,
        mesh=mesh,
        in_specs=(tokens, P(None), columns, columns, columns, P("tp", None)),
        out_specs=tokens,
        check_vma=False,
    )
```

```python
import functools

import jax
import jax.numpy as jnp
import numpy as np
from jax import lax
from jax.experimental import pallas as pl
from jax.experimental.pallas import tpu as pltpu
from jax.sharding import PartitionSpec as P

MESH = pl.DeviceIdType.MESH
NEG = -1e30
HIDDEN = 2 * NEG
LOG2E = 1.4426950408889634
HEAD = 128
THETA = 10000
N = 3
BLK = 256
ROWS = 512
NBLK = 16
D = 2048
W = N * HEAD
VR = 144
MR = HEAD + 8


def _dot(a, b, ca, cb):
    return lax.dot_general(a, b, (((ca,), (cb,)), ((), ())), preferred_element_type=jnp.float32)


def _rope_tables():
    half = HEAD // 2
    freq = THETA ** (-np.arange(half, dtype=np.float64) / half)
    sign = np.concatenate([-np.ones(half), np.ones(half)])
    def table(pos):
        ang = pos[:, None] * np.concatenate([freq, freq])
        return np.cos(ang).astype(np.float32), (np.sin(ang) * sign).astype(np.float32)
    lo = np.stack(table(np.arange(BLK, dtype=np.float64)))
    hi = np.stack(table(np.arange(NBLK, dtype=np.float64) * BLK))
    return lo, hi


def _place(me):
    core = me % 2
    y = (me // 2) % 2
    x = me // 4
    base = me - core
    xn = base + 4 - 8 * x
    yn = base + 2 - 4 * y
    dg = xn + 2 - 4 * y
    return core, base, xn, yn, dg


def _block(me, k, side):
    core, base, xn, yn, dg = _place(me)
    odd = k % 2
    flip = side + odd - 2 * side * odd
    near = jnp.where(side == 0, xn, yn) if not isinstance(side, int) else (xn if side == 0 else yn)
    dev = jnp.where(k < 1, me, jnp.where(k < 2, me + 1 - 2 * core, jnp.where(k < 6, near + flip, dg + 1 - flip)))
    half = jnp.where((k == 2) | (k == 3), 1 - side, side)
    return 2 * dev + half


def kernel(x_hbm, gain_ref, wq_ref, wk_ref, wv_ref, wo_ref, lo_hbm, hi_ref, y_ref,
           x_ref, lo_ref, a_s, w_s, q_s, k_s, v_s, top_s, mix_s, wo_s, seen_s, part_s, sum_s, wsem, send, recv, send2, recv2, lsem):
    me = lax.axis_index("tp")
    core, base, xn, yn, dg = _place(me)
    partner = base + 1 - core
    link = jnp.where(core == 0, xn, yn + 1)
    first = 1 - core

    def fetch(half, sem):
        rows = pl.ds(pl.multiple_of(half * BLK, BLK), BLK)
        return pltpu.make_async_copy(x_hbm.at[rows, :], x_ref.at[rows, :], wsem.at[sem])

    fetch(first, 4).start()
    fetch(1 - first, 5).start()

    barrier = pltpu.get_barrier_semaphore()
    for other in (partner, xn, xn + 1, yn, yn + 1):
        pl.semaphore_signal(barrier, inc=1, device_id={"tp": other}, device_id_type=MESH)

    loads = [pltpu.make_async_copy(w, w_s.at[:, pl.ds(i * W, W)], wsem.at[i]) for i, w in enumerate((wq_ref, wk_ref, wv_ref))]
    loads.append(pltpu.make_async_copy(lo_hbm, lo_ref, wsem.at[6]))
    for c in loads:
        c.start()
    wo_mine = wo_s.at[pl.ds(pl.multiple_of((2 + core) * W, W), W), :]
    wo_load = pltpu.make_async_copy(wo_ref, wo_mine, wsem.at[3])
    wo_load.start()

    def slot(s):
        return a_s.at[pl.ds(pl.multiple_of(s * BLK, BLK), BLK), :]

    def remote(src, dst, sem, dev):
        return pltpu.make_async_remote_copy(src_ref=slot(src), dst_ref=slot(dst), send_sem=send.at[sem], recv_sem=recv.at[dst],
                                            device_id={"tp": dev}, device_id_type=MESH)

    def send_wo(src, dst, sem, dev):
        at = lambda i: wo_s.at[pl.ds(pl.multiple_of(i * W, W), W), :]
        return pltpu.make_async_remote_copy(src_ref=at(src), dst_ref=at(dst), send_sem=send2.at[sem], recv_sem=recv2.at[dst],
                                            device_id={"tp": dev}, device_id_type=MESH)

    def arrived(s):
        return pltpu.make_async_remote_copy(src_ref=slot(s), dst_ref=slot(s), send_sem=send.at[0], recv_sem=recv.at[s],
                                            device_id={"tp": partner}, device_id_type=MESH).wait_recv()

    def wo_arrived(i):
        send_wo(i, i, 0, partner).wait_recv()

    gain = gain_ref[...].astype(jnp.float32).reshape(1, D)

    def norm(start, count):
        def rows(i, _):
            at = pl.ds(pl.multiple_of(start + i * 16, 16), 16)
            wide = x_ref[at, :].astype(jnp.float32)
            scale = lax.rsqrt(jnp.mean(wide * wide, -1, keepdims=True) + 1e-6)
            a_s[at, :] = (wide * scale * gain).astype(jnp.bfloat16)
        lax.fori_loop(0, count // 16, rows, None, unroll=8 if count == 256 else 2)

    fetch(first, 4).wait()
    norm(first * BLK, BLK)
    fetch(1 - first, 5).wait()
    pl.semaphore_wait(barrier, 5)
    norm((1 - first) * BLK, 32)
    remote(first, 4 + core, 2, link).start()
    remote(first, 2 + first, 0, partner).start()
    norm((1 - first) * BLK + 32, BLK - 32)
    v_s[:, :, HEAD:, :] = jnp.ones((NBLK, N, VR - HEAD, BLK), jnp.bfloat16)
    top_s[...] = jnp.full(top_s.shape, NEG, jnp.float32)

    def clear(i, _):
        mix_s[pl.ds(pl.multiple_of(i * MR, MR), MR), :] = jnp.zeros((MR, BLK), jnp.float32)

    lax.fori_loop(0, NBLK * N, clear, None)
    remote(1 - first, 3 - first, 1, partner).start()
    for c in loads:
        c.wait()
    wo_load.wait()
    send_wo(2 + core, 2 + core, 0, partner).start()

    scale_e = HEAD ** -0.5 * LOG2E

    def project(k, blocks):
        here = pl.ds(pl.multiple_of(k * ROWS, ROWS), ROWS)
        tables = []
        for b in blocks:
            ch, sh = hi_ref[0, pl.ds(b, 1), :], hi_ref[1, pl.ds(b, 1), :]
            cl, sl = lo_ref[0], lo_ref[1]
            tables.append((ch * cl - sh * sl, sh * cl + ch * sl))
        for g in range(0, 3 * N, 2):
            width = min(2, 3 * N - g) * HEAD
            out = _dot(a_s[here, :], w_s[:, g * HEAD : g * HEAD + width], 1, 0).astype(jnp.bfloat16)
            for i in range(width // HEAD):
                kind, n = divmod(g + i, N)
                for b, block in enumerate(blocks):
                    t = out[b * BLK : (b + 1) * BLK, i * HEAD : (i + 1) * HEAD]
                    if kind == 2:
                        v_s[block, n, :HEAD, :] = t.T
                    else:
                        t = t.astype(jnp.float32)
                        t = t * tables[b][0] + pltpu.roll(t, HEAD // 2, 1) * tables[b][1]
                        (q_s if kind == 0 else k_s)[block, n] = t.astype(jnp.bfloat16)

    def attend(pairs):
        strips = [(q, k, masked, n) for q, k, masked in pairs for n in range(N)]
        scores = [_dot(k_s[k, n], q_s[q, n], 1, 1) for q, k, _, n in strips]
        if any(masked for _, _, masked in pairs):
            ok = lax.broadcasted_iota(jnp.int32, (BLK, BLK), 1) >= lax.broadcasted_iota(jnp.int32, (BLK, BLK), 0)
        for (q, k, masked, n), s in zip(strips, scores):
            if masked:
                s = jnp.where(ok, s, HIDDEN)
            old = top_s[q, n : n + 1, :]
            top = jnp.maximum(old, s.max(axis=0, keepdims=True))
            top_s[q, n : n + 1, :] = top
            p = jnp.exp2((s - top) * scale_e).astype(jnp.bfloat16)
            keep = jnp.exp2((old - top) * scale_e)
            mix = pl.ds(pl.multiple_of((q * N + n) * MR, 8), MR)
            mix_s[mix, :] = mix_s[mix, :] * keep + _dot(v_s[k, n], p, 1, 0)[:MR, :]

    def event(k, _):
        b0, b1 = _block(me, k, 0), _block(me, k, 1)

        @pl.when(k >= 2)
        def _():
            arrived(2 * k + 1 - core)

            @pl.when(k < 4)
            def _():
                remote(2 * k + 1 - core, 2 * k + 8 + core, 4 + k, link).start()

            @pl.when(k == 3)
            def _():
                wo_arrived(3 - core)
                send_wo(2 + core, 5 * core, 1, link).start()
                send_wo(3 - core, 1 + 3 * core, 2, link).start()

        project(k, (b0, b1))

        @pl.when(k == 0)
        def _():
            arrived(2 + first)
            remote(2 + first, 6 + core, 3, link).start()
            remote(1 - first, 8 + core, 4, link).start()
            arrived(3 - first)
            remote(3 - first, 10 + core, 5, link).start()

        def older(j, _):
            pairs = []
            for new in (b0, b1):
                for side in (0, 1):
                    b = _block(me, j, side)
                    pairs.append((jnp.maximum(new, b), jnp.minimum(new, b), False))
            attend(pairs)

        lax.fori_loop(0, k, older, None)

        @pl.when((k >= 1) & (k < 7))
        def _():
            arrived(2 * k + 2 + core)
            remote(2 * k + 2 + core, 2 * k + 2 + core, 7 + k, partner).start()

        attend([(jnp.maximum(b0, b1), jnp.minimum(b0, b1), False), (b0, b0, True), (b1, b1, True)])

    lax.fori_loop(0, 8, event, None)

    def finish(b):
        rows = pl.ds(pl.multiple_of(b * BLK, BLK), BLK)
        for n in range(N):
            at = (b * N + n) * MR
            out = mix_s[pl.ds(pl.multiple_of(at, 8), HEAD), :] * (1 / mix_s[pl.ds(pl.multiple_of(at + HEAD, 8), 1), :])
            seen_s[rows, n * HEAD : (n + 1) * HEAD] = out.astype(jnp.bfloat16).T

    def seen(dev, half):
        return seen_s.at[pl.ds(pl.multiple_of((2 * dev + half) * BLK, BLK), BLK), :]

    def part(i, own, c):
        left = own == (i >= 2)
        return part_s.at[i, :, pl.ds(pl.multiple_of(c * W + (0 if left else 2 * W), HEAD), W)]

    def hand(src, i, own, sem, arrival, dev):
        return pltpu.make_async_remote_copy(src_ref=src, dst_ref=part(i, own, core), send_sem=send2.at[sem], recv_sem=recv2.at[arrival],
                                            device_id={"tp": dev}, device_id_type=MESH)

    for c in (0, 1):
        finish(2 * (dg + c))
        finish(2 * (dg + c) + 1)
        hand(seen(dg + c, 0), 0, False, 5 + c, 6 + core, xn + c).start()
        hand(seen(dg + c, 1), 2, False, 7 + c, 10 + core, yn + c).start()
    for c in (0, 1):
        finish(2 * (xn + c))
        hand(seen(xn + c, 0), 1, False, 9 + c, 8 + core, xn + c).start()
        finish(2 * (yn + c) + 1)
        hand(seen(yn + c, 1), 3, False, 11 + c, 12 + core, yn + c).start()
    for c in (0, 1):
        finish(2 * (yn + c))
        finish(2 * (xn + c) + 1)
        finish(2 * (base + c))
        finish(2 * (base + c) + 1)
    wanted = ((yn, 0), (base, 0), (xn, 1), (base, 1))
    for i, (chip, half) in enumerate(wanted):
        hand(seen(chip + 1 - core, half), i, True, 13 + i, 14 + i, partner).start()
    local = [pltpu.make_async_copy(seen(chip + core, half), part(i, True, core), lsem.at[i]) for i, (chip, half) in enumerate(wanted)]
    for c in local:
        c.start()

    for i in (0, 1):
        piece = 4 * core + (core + i - 2 * core * i)
        wo_arrived(piece)
        send_wo(piece, piece, 3 + i, partner).start()
    for i in (0, 1):
        wo_arrived(4 - 4 * core + i)
    for i in range(14):
        remote(0, 0, i, partner).wait_send()

    def ready(i):
        local[i].wait()
        hand(part(i, True, 0), i, True, 0, 14 + i, partner).wait_recv()
        for c in (0, 1):
            hand(part(i, True, 0), i, False, 0, 6 + 2 * i + c, partner).wait_recv()

    def product(i, rows, columns):
        return _dot(part_s[i, rows, :], wo_s[0 if i < 2 else 2 * W : 4 * W if i < 2 else 6 * W, columns], 1, 0)

    PIECE = 128

    def give(i, piece, dev):
        at = pl.ds(PIECE * (i + piece), PIECE)
        return pltpu.make_async_remote_copy(src_ref=a_s.at[at, :], dst_ref=sum_s.at[at, :], send_sem=send2.at[17 + i + piece],
                                            recv_sem=recv2.at[18 + i + piece], device_id={"tp": dev}, device_id_type=MESH)

    WIDE = 512
    for i, dev in ((0, yn + core), (2, xn + core)):
        ready(i)
        for piece in (0, 1):
            def columns(n, _):
                at = pl.ds(pl.multiple_of(n * WIDE, WIDE), WIDE)
                a_s[PIECE * (i + piece) : PIECE * (i + piece + 1), at] = product(i, slice(PIECE * piece, PIECE * (piece + 1)), at).astype(jnp.bfloat16)
            lax.fori_loop(0, D // WIDE, columns, None)
            give(i, piece, dev).start()
    for i in (1, 3):
        ready(i)

        def columns(n, _):
            out = product(i, slice(None), pl.ds(pl.multiple_of(n * BLK, BLK), BLK))
            mix_s[pl.ds(pl.multiple_of(n * ROWS + (i - 1) * PIECE, BLK), BLK), :] = out

        lax.fori_loop(0, D // BLK, columns, None)

    for piece in (0, 1):
        for i in (0, 2):
            give(i, piece, partner).wait_recv()
            r = PIECE * (i + piece)
            for n in range(D // BLK):
                at = slice(n * BLK, (n + 1) * BLK)
                total = mix_s[n * ROWS + r : n * ROWS + r + PIECE, :] + sum_s[r : r + PIECE, at].astype(jnp.float32)
                y_ref[r : r + PIECE, at] = (x_ref[r : r + PIECE, at].astype(jnp.float32) + total).astype(jnp.bfloat16)

    for i in range(5):
        send_wo(0, 0, i, partner).wait_send()
    for i in range(5, 17):
        hand(seen(0, 0), 0, True, i, 14, partner).wait_send()
    for i in (0, 2):
        for piece in (0, 1):
            give(i, piece, partner).wait_send()


def solution(mesh):
    def step(x, gain, wq, wk, wv, wo):
        lo, hi = _rope_tables()
        any_space = pl.BlockSpec(memory_space=pl.ANY)
        vmem = pl.BlockSpec(memory_space=pltpu.VMEM)
        return pl.pallas_call(
            kernel,
            out_shape=pltpu.VMEM((ROWS, D), jnp.bfloat16),
            in_specs=[any_space, vmem, any_space, any_space, any_space, any_space, any_space, vmem],
            out_specs=vmem,
            scratch_shapes=[
                pltpu.VMEM((ROWS, D), jnp.bfloat16),
                pltpu.VMEM((2, BLK, HEAD), jnp.float32),
                pltpu.VMEM((NBLK * BLK, D), jnp.bfloat16),
                pltpu.VMEM((D, 3 * W), jnp.bfloat16),
                pltpu.VMEM((NBLK, N, BLK, HEAD), jnp.bfloat16),
                pltpu.VMEM((NBLK, N, BLK, HEAD), jnp.bfloat16),
                pltpu.VMEM((NBLK, N, VR, BLK), jnp.bfloat16),
                pltpu.VMEM((NBLK, 8, BLK), jnp.float32),
                pltpu.VMEM((NBLK * N * MR, BLK), jnp.float32),
                pltpu.VMEM((6 * W, D), jnp.bfloat16),
                pltpu.VMEM((NBLK * BLK, W), jnp.bfloat16),
                pltpu.VMEM((4, BLK, 4 * W), jnp.bfloat16),
                pltpu.VMEM((ROWS, D), jnp.bfloat16),
                pltpu.SemaphoreType.DMA((7,)),
                pltpu.SemaphoreType.DMA((14,)),
                pltpu.SemaphoreType.DMA((16,)),
                pltpu.SemaphoreType.DMA((21,)),
                pltpu.SemaphoreType.DMA((22,)),
                pltpu.SemaphoreType.DMA((4,)),
            ],
            compiler_params=pltpu.CompilerParams(collective_id=0, has_side_effects=True, vmem_limit_bytes=61 * 2**20),
            cost_estimate=pl.CostEstimate(flops=40 * 10**9, bytes_accessed=10**7, transcendentals=3 * 10**7),
        )(x, gain, wq, wk, wv, wo, jnp.asarray(lo), jnp.asarray(hi))

    tokens, columns = P(("dp", "tp"), None), P(None, "tp")
    return jax.shard_map(
        step,
        mesh=mesh,
        in_specs=(tokens, P(None), columns, columns, columns, P("tp", None)),
        out_specs=tokens,
        check_vma=False,
    )
```

```python
import functools

import jax
import jax.numpy as jnp
import numpy as np
from jax import lax
from jax.experimental import pallas as pl
from jax.experimental.pallas import tpu as pltpu
from jax.sharding import PartitionSpec as P

MESH = pl.DeviceIdType.MESH
NEG = -1e30
HIDDEN = 2 * NEG
LOG2E = 1.4426950408889634
HEAD = 128
THETA = 10000
WIDE = 512
PIECE = 128
AHEAD = 4
N = 3
BLK = 256
ROWS = 512
NBLK = 16
D = 2048
W = N * HEAD
VR = 144
MR = HEAD + 8


def _dot(a, b, ca, cb):
    return lax.dot_general(a, b, (((ca,), (cb,)), ((), ())), preferred_element_type=jnp.float32)


def _rope_tables():
    half = HEAD // 2
    freq = THETA ** (-np.arange(half, dtype=np.float64) / half)
    sign = np.concatenate([-np.ones(half), np.ones(half)])
    def table(pos):
        ang = pos[:, None] * np.concatenate([freq, freq])
        return np.cos(ang).astype(np.float32), (np.sin(ang) * sign).astype(np.float32)
    lo = np.stack(table(np.arange(BLK, dtype=np.float64)))
    hi = np.stack(table(np.arange(NBLK, dtype=np.float64) * BLK))
    return lo, hi


def _place(me):
    core = me % 2
    y = (me // 2) % 2
    x = me // 4
    base = me - core
    xn = base + 4 - 8 * x
    yn = base + 2 - 4 * y
    dg = xn + 2 - 4 * y
    return core, base, xn, yn, dg


def _block(me, k, side):
    core, base, xn, yn, dg = _place(me)
    odd = k % 2
    flip = side + odd - 2 * side * odd
    near = jnp.where(side == 0, xn, yn) if not isinstance(side, int) else (xn if side == 0 else yn)
    dev = jnp.where(k < 1, me, jnp.where(k < 2, me + 1 - 2 * core, jnp.where(k < 6, near + flip, dg + 1 - flip)))
    half = jnp.where((k == 2) | (k == 3), 1 - side, side)
    return 2 * dev + half


def kernel(x_hbm, gain_ref, wq_ref, wk_ref, wv_ref, wo_ref, lo_hbm, hi_ref, y_ref,
           x_ref, lo_ref, a_s, w_s, q_s, k_s, v_s, top_s, mix_s, wo_s, seen_s, part_s, sum_s, wsem, send, recv, send2, recv2, lsem):
    me = lax.axis_index("tp")
    core, base, xn, yn, dg = _place(me)
    partner = base + 1 - core
    link = jnp.where(core == 0, xn, yn + 1)
    first = 1 - core

    def fetch(half, sem):
        rows = pl.ds(pl.multiple_of(half * BLK, BLK), BLK)
        return pltpu.make_async_copy(x_hbm.at[rows, :], x_ref.at[rows, :], wsem.at[sem])

    fetch(first, 4).start()
    fetch(1 - first, 5).start()

    barrier = pltpu.get_barrier_semaphore()
    for other in (partner, xn + core, yn, yn + 1):
        pl.semaphore_signal(barrier, inc=1, device_id={"tp": other}, device_id_type=MESH)

    loads = [pltpu.make_async_copy(w, w_s.at[:, pl.ds(i * W, W)], wsem.at[i]) for i, w in enumerate((wq_ref, wk_ref, wv_ref))]
    loads.append(pltpu.make_async_copy(lo_hbm, lo_ref, wsem.at[6]))
    for c in loads:
        c.start()
    wo_mine = wo_s.at[pl.ds(pl.multiple_of(core * W, W), W), :]
    wo_load = pltpu.make_async_copy(wo_ref, wo_mine, wsem.at[3])
    wo_load.start()

    def slot(s):
        return a_s.at[pl.ds(pl.multiple_of(s * BLK, BLK), BLK), :]

    def remote(src, dst, sem, dev):
        return pltpu.make_async_remote_copy(src_ref=slot(src), dst_ref=slot(dst), send_sem=send.at[sem], recv_sem=recv.at[dst],
                                            device_id={"tp": dev}, device_id_type=MESH)

    def send_wo(src, dst, sem, arrival, dev, q=None):
        columns = slice(None) if q is None else pl.ds(pl.multiple_of(q * WIDE, WIDE), WIDE)
        at = lambda i: wo_s.at[pl.ds(pl.multiple_of(i * W, W), W), columns]
        return pltpu.make_async_remote_copy(src_ref=at(src), dst_ref=at(dst), send_sem=send2.at[sem], recv_sem=recv2.at[arrival],
                                            device_id={"tp": dev}, device_id_type=MESH)

    def wo_out(q):
        return send_wo(core, 2 + core, 1 + q, 2 + 2 * q + core, yn + core, q)

    def wo_on(q):
        return send_wo(2 + core, 2 + core, 5 + q, 2 + 2 * q + core, partner, q)

    def wo_in(q):
        send_wo(2 + core, 2 + core, 0, 2 + 2 * q + core, partner, q).wait_recv()
        wo_on(q).start()

    def wo_all(q):
        send_wo(3 - core, 3 - core, 0, 3 + 2 * q - core, partner, q).wait_recv()

    def arrived(s):
        return pltpu.make_async_remote_copy(src_ref=slot(s), dst_ref=slot(s), send_sem=send.at[0], recv_sem=recv.at[s],
                                            device_id={"tp": partner}, device_id_type=MESH).wait_recv()

    gain = gain_ref[...].astype(jnp.float32).reshape(1, D)

    def norm(start, count):
        def rows(i, _):
            at = pl.ds(pl.multiple_of(start + i * 16, 16), 16)
            wide = x_ref[at, :].astype(jnp.float32)
            scale = lax.rsqrt(jnp.mean(wide * wide, -1, keepdims=True) + 1e-6)
            a_s[at, :] = (wide * scale * gain).astype(jnp.bfloat16)
        lax.fori_loop(0, count // 16, rows, None, unroll=8 if count == 256 else 2)

    fetch(first, 4).wait()
    norm(first * BLK, BLK)
    fetch(1 - first, 5).wait()
    pl.semaphore_wait(barrier, 4)
    norm((1 - first) * BLK, 32)
    remote(first, 4 + core, 2, link).start()
    remote(first, 2 + first, 0, partner).start()
    norm((1 - first) * BLK + 32, BLK - 32)
    v_s[:, :, HEAD:, :] = jnp.ones((NBLK, N, VR - HEAD, BLK), jnp.bfloat16)
    top_s[...] = jnp.full(top_s.shape, NEG, jnp.float32)

    def clear(i, _):
        mix_s[pl.ds(pl.multiple_of(i * MR, MR), MR), :] = jnp.zeros((MR, BLK), jnp.float32)

    lax.fori_loop(0, NBLK * N, clear, None)
    remote(1 - first, 3 - first, 1, partner).start()
    for c in loads:
        c.wait()
    wo_load.wait()
    send_wo(core, core, 0, core, partner).start()

    scale_e = HEAD ** -0.5 * LOG2E

    def project(k, blocks):
        here = pl.ds(pl.multiple_of(k * ROWS, ROWS), ROWS)
        tables = []
        for b in blocks:
            ch, sh = hi_ref[0, pl.ds(b, 1), :], hi_ref[1, pl.ds(b, 1), :]
            cl, sl = lo_ref[0], lo_ref[1]
            tables.append((ch * cl - sh * sl, sh * cl + ch * sl))
        for g in range(0, 3 * N, 2):
            width = min(2, 3 * N - g) * HEAD
            out = _dot(a_s[here, :], w_s[:, g * HEAD : g * HEAD + width], 1, 0).astype(jnp.bfloat16)
            for i in range(width // HEAD):
                kind, n = divmod(g + i, N)
                for b, block in enumerate(blocks):
                    t = out[b * BLK : (b + 1) * BLK, i * HEAD : (i + 1) * HEAD]
                    if kind == 2:
                        v_s[block, n, :HEAD, :] = t.T
                    else:
                        t = t.astype(jnp.float32)
                        t = t * tables[b][0] + pltpu.roll(t, HEAD // 2, 1) * tables[b][1]
                        (q_s if kind == 0 else k_s)[block, n] = t.astype(jnp.bfloat16)

    def attend(pairs):
        strips = [(q, k, masked, n) for q, k, masked in pairs for n in range(N)]
        if any(masked for _, _, masked in pairs):
            ok = lax.broadcasted_iota(jnp.int32, (BLK, BLK), 1) >= lax.broadcasted_iota(jnp.int32, (BLK, BLK), 0)

        def score(q, k, masked, n):
            return _dot(k_s[k, n], q_s[q, n], 1, 1)

        ahead = [score(*strip) for strip in strips[:AHEAD]]
        for i, (q, k, masked, n) in enumerate(strips):
            if i + AHEAD < len(strips):
                ahead.append(score(*strips[i + AHEAD]))
            s = ahead.pop(0)
            if masked:
                s = jnp.where(ok, s, HIDDEN)
            old = top_s[q, n : n + 1, :]
            top = jnp.maximum(old, s.max(axis=0, keepdims=True))
            top_s[q, n : n + 1, :] = top
            p = jnp.exp2((s - top) * scale_e).astype(jnp.bfloat16)
            keep = jnp.exp2((old - top) * scale_e)
            mix = pl.ds(pl.multiple_of((q * N + n) * MR, 8), MR)
            mix_s[mix, :] = mix_s[mix, :] * keep + _dot(v_s[k, n], p, 1, 0)[:MR, :]

    def both(new, old):
        return jnp.maximum(new, old), jnp.minimum(new, old), False

    def event(k, _):
        b0, b1 = _block(me, k, 0), _block(me, k, 1)

        @pl.when(k >= 2)
        def _():
            arrived(2 * k + 1 - core)

            @pl.when(k < 4)
            def _():
                remote(2 * k + 1 - core, 2 * k + 8 + core, 4 + k, link).start()

            @pl.when((k == 3) & (core == 1))
            def _():
                wo_out(0).start()
                wo_out(1).start()

        project(k, (b0, b1))

        @pl.when(k == 0)
        def _():
            arrived(2 + first)
            remote(2 + first, 6 + core, 3, link).start()
            remote(1 - first, 8 + core, 4, link).start()
            arrived(3 - first)
            remote(3 - first, 10 + core, 5, link).start()

        def older(j, _):
            pairs = []
            for new in (b0, b1):
                for side in (0, 1):
                    pairs.append(both(new, _block(me, j, side)))
            attend(pairs)

        lax.fori_loop(0, k, older, None)

        @pl.when(k >= 1)
        def _():
            arrived(2 * k + 2 + core)
            remote(2 * k + 2 + core, 2 * k + 2 + core, 7 + k, partner).start()

        attend([both(b0, b1), (b0, b0, True), (b1, b1, True)])

    lax.fori_loop(0, 7, event, None)

    arrived(15 - core)

    @pl.when(core == 0)
    def _():
        wo_out(0).start()
        wo_out(1).start()

    b0, b1 = _block(me, 7, 0), _block(me, 7, 1)
    project(7, (b0, b1))

    def against(new):
        def four(i, _):
            attend([both(new, _block(me, 2 * i + j, side)) for j in (0, 1) for side in (0, 1)])

        lax.fori_loop(0, 3, four, None)

    against(b0)
    attend([both(b0, _block(me, 6, 0)), both(b0, _block(me, 6, 1)), (b0, b0, True)])

    def finish(b):
        rows = pl.ds(pl.multiple_of(b * BLK, BLK), BLK)
        for n in range(N):
            at = (b * N + n) * MR
            out = mix_s[pl.ds(pl.multiple_of(at, 8), HEAD), :] * (1 / mix_s[pl.ds(pl.multiple_of(at + HEAD, 8), 1), :])
            seen_s[rows, n * HEAD : (n + 1) * HEAD] = out.astype(jnp.bfloat16).T

    def piece(dev, r, count=PIECE):
        return seen_s.at[pl.ds(pl.multiple_of(dev * ROWS + r * PIECE, PIECE), count), :]

    def part(i, theirs, c, r, count=PIECE):
        return part_s.at[i, pl.ds(pl.multiple_of(r * PIECE, PIECE), count), pl.ds(pl.multiple_of((2 * theirs + c) * W, HEAD), W)]

    def across(i, r, c, chip):
        return pltpu.make_async_remote_copy(src_ref=piece(chip + c, r), dst_ref=part(i, 1, core, r), send_sem=send2.at[17 + 8 * i + 2 * r + c],
                                            recv_sem=recv2.at[10 + 8 * i + 2 * r + core], device_id={"tp": yn + c}, device_id_type=MESH)

    def across_wait(i, r):
        for c in (0, 1):
            pltpu.make_async_remote_copy(src_ref=part(i, 1, c, r), dst_ref=part(i, 1, c, r), send_sem=send2.at[0],
                                         recv_sem=recv2.at[10 + 8 * i + 2 * r + c], device_id={"tp": partner}, device_id_type=MESH).wait_recv()

    def hand(i, chip):
        return pltpu.make_async_remote_copy(src_ref=piece(chip + 1 - core, 0, ROWS), dst_ref=part(i, 0, core, 0, ROWS), send_sem=send2.at[33 + i],
                                            recv_sem=recv2.at[26 + i], device_id={"tp": partner}, device_id_type=MESH)

    def keep(i, chip):
        return pltpu.make_async_copy(piece(chip + core, 0, ROWS), part(i, 0, core, 0, ROWS), lsem.at[i])

    def give(q, r):
        at = (pl.ds(pl.multiple_of(r * PIECE, PIECE), PIECE), pl.ds(pl.multiple_of(q * WIDE, WIDE), WIDE))
        return pltpu.make_async_remote_copy(src_ref=a_s.at[at], dst_ref=sum_s.at[at], send_sem=send2.at[35 + 4 * q + r],
                                            recv_sem=recv2.at[28 + 4 * q + r], device_id={"tp": xn + core}, device_id_type=MESH)

    def partial_sum(q, r):
        rows, columns = pl.ds(pl.multiple_of(r * PIECE, PIECE), PIECE), pl.ds(pl.multiple_of(q * WIDE, WIDE), WIDE)
        a_s[rows, columns] = _dot(part_s[0, rows, :], wo_s[:, columns], 1, 0).astype(jnp.bfloat16)
        give(q, r).start()

    def far(half):
        for c in (0, 1):
            finish(2 * (dg + c) + half)
        for r in (2 * half, 2 * half + 1):
            for c in (0, 1):
                across(0, r, c, dg).start()

    far(0)
    against(b1)
    attend([both(b1, _block(me, 6, 0)), both(b1, _block(me, 6, 1)), both(b1, b0), (b1, b1, True)])
    for b in range(4):
        finish(2 * xn + b)
    hand(0, xn).start()
    keep(0, xn).start()
    far(1)
    wo_out(2).start()
    wo_out(3).start()
    for b in range(4):
        finish(2 * yn + b)
    for r in range(4):
        for c in (0, 1):
            across(1, r, c, yn).start()
    for b in range(4):
        finish(2 * base + b)
    hand(1, base).start()
    keep(1, base).start()
    wo_in(0)
    wo_in(1)
    for i in range(14):
        remote(0, 0, i, partner).wait_send()
    send_wo(1 - core, 1 - core, 0, 1 - core, partner).wait_recv()
    wo_all(0)
    wo_all(1)
    keep(0, xn).wait()
    hand(0, xn).wait_recv()

    def early(r, _):
        across_wait(0, r)
        partial_sum(0, r)
        partial_sum(1, r)

    lax.fori_loop(0, 4, early, None)
    keep(1, base).wait()
    hand(1, base).wait_recv()

    def ours(n, _):
        out = _dot(part_s[1, :, : 2 * W], wo_s[: 2 * W, pl.ds(pl.multiple_of(n * BLK, BLK), BLK)], 1, 0)
        mix_s[pl.ds(pl.multiple_of(n * ROWS, ROWS), ROWS), :] = out

    lax.fori_loop(0, D // BLK, ours, None)
    for q in (2, 3):
        wo_in(q)
        wo_all(q)

        def late(r, _):
            partial_sum(q, r)

        lax.fori_loop(0, 4, late, None)

    def last(r, _):
        rows = pl.ds(pl.multiple_of(r * PIECE, PIECE), PIECE)
        across_wait(1, r)
        for n in range(D // BLK):
            at = pl.ds(pl.multiple_of(n * ROWS + r * PIECE, PIECE), PIECE)
            mix_s[at, :] += _dot(part_s[1, rows, 2 * W :], wo_s[2 * W :, n * BLK : (n + 1) * BLK], 1, 0)
        for q in range(4):
            give(q, r).wait_recv()
        for n in range(D // BLK):
            at = slice(n * BLK, (n + 1) * BLK)
            total = mix_s[pl.ds(pl.multiple_of(n * ROWS + r * PIECE, PIECE), PIECE), :] + sum_s[rows, at].astype(jnp.float32)
            y_ref[rows, at] = (x_ref[rows, at].astype(jnp.float32) + total).astype(jnp.bfloat16)

    lax.fori_loop(0, 4, last, None)

    send_wo(core, core, 0, core, partner).wait_send()

    for q in range(4):
        wo_out(q).wait_send()
        wo_on(q).wait_send()

    def sent(r, _):
        for c in (0, 1):
            across(0, r, c, dg).wait_send()
            across(1, r, c, yn).wait_send()
        for q in range(4):
            give(q, r).wait_send()

    lax.fori_loop(0, 4, sent, None)
    hand(0, xn).wait_send()
    hand(1, base).wait_send()


def solution(mesh):
    def step(x, gain, wq, wk, wv, wo):
        lo, hi = _rope_tables()
        any_space = pl.BlockSpec(memory_space=pl.ANY)
        vmem = pl.BlockSpec(memory_space=pltpu.VMEM)
        return pl.pallas_call(
            kernel,
            out_shape=pltpu.VMEM((ROWS, D), jnp.bfloat16),
            in_specs=[any_space, vmem, any_space, any_space, any_space, any_space, any_space, vmem],
            out_specs=vmem,
            scratch_shapes=[
                pltpu.VMEM((ROWS, D), jnp.bfloat16),
                pltpu.VMEM((2, BLK, HEAD), jnp.float32),
                pltpu.VMEM((NBLK * BLK, D), jnp.bfloat16),
                pltpu.VMEM((D, 3 * W), jnp.bfloat16),
                pltpu.VMEM((NBLK, N, BLK, HEAD), jnp.bfloat16),
                pltpu.VMEM((NBLK, N, BLK, HEAD), jnp.bfloat16),
                pltpu.VMEM((NBLK, N, VR, BLK), jnp.bfloat16),
                pltpu.VMEM((NBLK, 8, BLK), jnp.float32),
                pltpu.VMEM((NBLK * N * MR, BLK), jnp.float32),
                pltpu.VMEM((4 * W, D), jnp.bfloat16),
                pltpu.VMEM((NBLK * BLK, W), jnp.bfloat16),
                pltpu.VMEM((2, ROWS, 4 * W), jnp.bfloat16),
                pltpu.VMEM((ROWS, D), jnp.bfloat16),
                pltpu.SemaphoreType.DMA((7,)),
                pltpu.SemaphoreType.DMA((14,)),
                pltpu.SemaphoreType.DMA((16,)),
                pltpu.SemaphoreType.DMA((51,)),
                pltpu.SemaphoreType.DMA((44,)),
                pltpu.SemaphoreType.DMA((2,)),
            ],
            compiler_params=pltpu.CompilerParams(collective_id=0, has_side_effects=True, vmem_limit_bytes=61 * 2**20),
            cost_estimate=pl.CostEstimate(flops=40 * 10**9, bytes_accessed=10**7, transcendentals=3 * 10**7),
        )(x, gain, wq, wk, wv, wo, jnp.asarray(lo), jnp.asarray(hi))

    tokens, columns = P(("dp", "tp"), None), P(None, "tp")
    return jax.shard_map(
        step,
        mesh=mesh,
        in_specs=(tokens, P(None), columns, columns, columns, P("tp", None)),
        out_specs=tokens,
        check_vma=False,
    )
```

```python
import functools

import jax
import jax.numpy as jnp
import numpy as np
from jax import lax
from jax.experimental import pallas as pl
from jax.experimental.pallas import tpu as pltpu
from jax.sharding import PartitionSpec as P

MESH = pl.DeviceIdType.MESH
NEG = -1e30
HIDDEN = 2 * NEG
LOG2E = 1.4426950408889634
HEAD = 128
THETA = 10000
WIDE = 512
PIECE = 128
AHEAD = 4
N = 3
BLK = 256
ROWS = 512
NBLK = 16
D = 2048
W = N * HEAD
VR = 144
MR = HEAD + 8


def _dot(a, b, ca, cb):
    return lax.dot_general(a, b, (((ca,), (cb,)), ((), ())), preferred_element_type=jnp.float32)


def _rope_tables():
    half = HEAD // 2
    freq = THETA ** (-np.arange(half, dtype=np.float64) / half)
    sign = np.concatenate([-np.ones(half), np.ones(half)])
    def table(pos):
        ang = pos[:, None] * np.concatenate([freq, freq])
        return np.cos(ang).astype(np.float32), (np.sin(ang) * sign).astype(np.float32)
    lo = np.stack(table(np.arange(BLK, dtype=np.float64)))
    hi = np.stack(table(np.arange(NBLK, dtype=np.float64) * BLK))
    return lo, hi


def _place(me):
    core = me % 2
    y = (me // 2) % 2
    x = me // 4
    base = me - core
    xn = base + 4 - 8 * x
    yn = base + 2 - 4 * y
    dg = xn + 2 - 4 * y
    return core, base, xn, yn, dg


def _block(me, k, side):
    core, base, xn, yn, dg = _place(me)
    odd = k % 2
    flip = side + odd - 2 * side * odd
    near = jnp.where(side == 0, xn, yn) if not isinstance(side, int) else (xn if side == 0 else yn)
    dev = jnp.where(k < 1, me, jnp.where(k < 2, me + 1 - 2 * core, jnp.where(k < 6, near + flip, dg + 1 - flip)))
    half = jnp.where((k == 2) | (k == 3), 1 - side, side)
    return 2 * dev + half


def kernel(x_hbm, gain_ref, wq_ref, wk_ref, wv_ref, wo_ref, lo_hbm, hi_ref, y_ref,
           x_ref, lo_ref, a_s, w_s, q_s, k_s, v_s, top_s, mix_s, wo_s, seen_s, part_s, sum_s, wsem, send, recv, send2, recv2, lsem):
    me = lax.axis_index("tp")
    core, base, xn, yn, dg = _place(me)
    partner = base + 1 - core
    link = jnp.where(core == 0, xn, yn + 1)
    first = 1 - core

    def fetch(half, sem):
        rows = pl.ds(pl.multiple_of(half * BLK, BLK), BLK)
        return pltpu.make_async_copy(x_hbm.at[rows, :], x_ref.at[rows, :], wsem.at[sem])

    fetch(first, 4).start()
    fetch(1 - first, 5).start()

    barrier = pltpu.get_barrier_semaphore()
    for other in (partner, xn + core, yn, yn + 1):
        pl.semaphore_signal(barrier, inc=1, device_id={"tp": other}, device_id_type=MESH)

    loads = [pltpu.make_async_copy(w, w_s.at[:, pl.ds(i * W, W)], wsem.at[i]) for i, w in enumerate((wq_ref, wk_ref, wv_ref))]
    loads.append(pltpu.make_async_copy(lo_hbm, lo_ref, wsem.at[6]))
    for c in loads:
        c.start()
    wo_mine = wo_s.at[pl.ds(pl.multiple_of(core * W, W), W), :]
    wo_load = pltpu.make_async_copy(wo_ref, wo_mine, wsem.at[3])
    wo_load.start()

    def slot(s):
        return a_s.at[pl.ds(pl.multiple_of(s * BLK, BLK), BLK), :]

    def remote(src, dst, sem, dev):
        return pltpu.make_async_remote_copy(src_ref=slot(src), dst_ref=slot(dst), send_sem=send.at[sem], recv_sem=recv.at[dst],
                                            device_id={"tp": dev}, device_id_type=MESH)

    def send_wo(src, dst, sem, arrival, dev, q=None):
        columns = slice(None) if q is None else pl.ds(pl.multiple_of(q * WIDE, WIDE), WIDE)
        at = lambda i: wo_s.at[pl.ds(pl.multiple_of(i * W, W), W), columns]
        return pltpu.make_async_remote_copy(src_ref=at(src), dst_ref=at(dst), send_sem=send2.at[sem], recv_sem=recv2.at[arrival],
                                            device_id={"tp": dev}, device_id_type=MESH)

    def wo_out(q):
        return send_wo(core, 2 + core, 1 + q, 2 + 2 * q + core, yn + core, q)

    def wo_on(q):
        return send_wo(2 + core, 2 + core, 5 + q, 2 + 2 * q + core, partner, q)

    def wo_in(q):
        send_wo(2 + core, 2 + core, 0, 2 + 2 * q + core, partner, q).wait_recv()
        wo_on(q).start()

    def wo_all(q):
        send_wo(3 - core, 3 - core, 0, 3 + 2 * q - core, partner, q).wait_recv()

    def half(src, dst, h, sem, arrival, dev):
        at = lambda i: a_s.at[pl.ds(pl.multiple_of(i * BLK + h * PIECE, PIECE), PIECE), :]
        return pltpu.make_async_remote_copy(src_ref=at(src), dst_ref=at(dst), send_sem=send.at[sem], recv_sem=recv.at[arrival],
                                            device_id={"tp": dev}, device_id_type=MESH)

    def arrived(s):
        return pltpu.make_async_remote_copy(src_ref=slot(s), dst_ref=slot(s), send_sem=send.at[0], recv_sem=recv.at[s],
                                            device_id={"tp": partner}, device_id_type=MESH).wait_recv()

    gain = gain_ref[...].astype(jnp.float32).reshape(1, D)

    def norm(start, count):
        def rows(i, _):
            at = pl.ds(pl.multiple_of(start + i * 16, 16), 16)
            wide = x_ref[at, :].astype(jnp.float32)
            scale = lax.rsqrt(jnp.mean(wide * wide, -1, keepdims=True) + 1e-6)
            a_s[at, :] = (wide * scale * gain).astype(jnp.bfloat16)
        lax.fori_loop(0, count // 16, rows, None, unroll=8 if count == 256 else 2)

    fetch(first, 4).wait()
    norm(first * BLK, BLK)
    fetch(1 - first, 5).wait()
    pl.semaphore_wait(barrier, 4)
    norm((1 - first) * BLK, 32)
    remote(first, 4 + core, 2, link).start()
    remote(first, 2 + first, 0, partner).start()
    norm((1 - first) * BLK + 32, BLK - 32)
    v_s[:, :, HEAD:, :] = jnp.ones((NBLK, N, VR - HEAD, BLK), jnp.bfloat16)
    top_s[...] = jnp.full(top_s.shape, NEG, jnp.float32)

    def clear(i, _):
        mix_s[pl.ds(pl.multiple_of(i * MR, MR), MR), :] = jnp.zeros((MR, BLK), jnp.float32)

    lax.fori_loop(0, NBLK * N, clear, None)
    remote(1 - first, 3 - first, 1, partner).start()
    for c in loads:
        c.wait()
    wo_load.wait()
    send_wo(core, core, 0, core, partner).start()

    scale_e = HEAD ** -0.5 * LOG2E

    def project(first_slot, blocks):
        here = pl.ds(pl.multiple_of(first_slot * BLK, BLK), BLK * len(blocks))
        tables = []
        for b in blocks:
            ch, sh = hi_ref[0, pl.ds(b, 1), :], hi_ref[1, pl.ds(b, 1), :]
            cl, sl = lo_ref[0], lo_ref[1]
            tables.append((ch * cl - sh * sl, sh * cl + ch * sl))
        for g in range(0, 3 * N, 2):
            width = min(2, 3 * N - g) * HEAD
            out = _dot(a_s[here, :], w_s[:, g * HEAD : g * HEAD + width], 1, 0).astype(jnp.bfloat16)
            for i in range(width // HEAD):
                kind, n = divmod(g + i, N)
                for b, block in enumerate(blocks):
                    t = out[b * BLK : (b + 1) * BLK, i * HEAD : (i + 1) * HEAD]
                    if kind == 2:
                        v_s[block, n, :HEAD, :] = t.T
                    else:
                        t = t.astype(jnp.float32)
                        t = t * tables[b][0] + pltpu.roll(t, HEAD // 2, 1) * tables[b][1]
                        (q_s if kind == 0 else k_s)[block, n] = t.astype(jnp.bfloat16)

    def attend(pairs):
        strips = [(q, k, masked, n) for q, k, masked in pairs for n in range(N)]
        if any(masked for _, _, masked in pairs):
            ok = lax.broadcasted_iota(jnp.int32, (BLK, BLK), 1) >= lax.broadcasted_iota(jnp.int32, (BLK, BLK), 0)

        def score(q, k, masked, n):
            return _dot(k_s[k, n], q_s[q, n], 1, 1)

        ahead = [score(*strip) for strip in strips[:AHEAD]]
        for i, (q, k, masked, n) in enumerate(strips):
            if i + AHEAD < len(strips):
                ahead.append(score(*strips[i + AHEAD]))
            s = ahead.pop(0)
            if masked:
                s = jnp.where(ok, s, HIDDEN)
            old = top_s[q, n : n + 1, :]
            top = jnp.maximum(old, s.max(axis=0, keepdims=True))
            top_s[q, n : n + 1, :] = top
            p = jnp.exp2((s - top) * scale_e).astype(jnp.bfloat16)
            keep = jnp.exp2((old - top) * scale_e)
            mix = pl.ds(pl.multiple_of((q * N + n) * MR, 8), MR)
            mix_s[mix, :] = mix_s[mix, :] * keep + _dot(v_s[k, n], p, 1, 0)[:MR, :]

    def both(new, old):
        return jnp.maximum(new, old), jnp.minimum(new, old), False

    def event(k, _):
        b0, b1 = _block(me, k, 0), _block(me, k, 1)

        @pl.when(k >= 2)
        def _():
            arrived(2 * k + 1 - core)

            @pl.when((k == 2) | ((k == 3) & (core == 0)))
            def _():
                remote(2 * k + 1 - core, 2 * k + 8 + core, 4 + k, link).start()

            @pl.when((k == 3) & (core == 1))
            def _():
                half(6, 15, 0, 7, 15, link).start()

            @pl.when((k == 4) & (core == 0))
            def _():
                half(9, 15, 1, 14, 16, link).start()

            @pl.when((k == 3) & (core == 1))
            def _():
                wo_out(0).start()
                wo_out(1).start()

        project(2 * k, (b0, b1))

        @pl.when(k == 0)
        def _():
            arrived(2 + first)
            remote(2 + first, 6 + core, 3, link).start()
            remote(1 - first, 8 + core, 4, link).start()
            arrived(3 - first)
            remote(3 - first, 10 + core, 5, link).start()

        def older(j, _):
            pairs = []
            for new in (b0, b1):
                for side in (0, 1):
                    pairs.append(both(new, _block(me, j, side)))
            attend(pairs)

        lax.fori_loop(0, k, older, None)

        @pl.when((k >= 1) & ((k < 6) | (core == 0)))
        def _():
            arrived(2 * k + 2 + core)
            remote(2 * k + 2 + core, 2 * k + 2 + core, 7 + k, partner).start()

        @pl.when((k == 6) & (core == 1))
        def _():
            half(15, 15, 0, 13, 15, partner).wait_recv()
            half(15, 15, 0, 13, 15, partner).start()

        attend([both(b0, b1), (b0, b0, True), (b1, b1, True)])

    lax.fori_loop(0, 7, event, None)

    @pl.when(core == 0)
    def _():
        wo_out(0).start()
        wo_out(1).start()

    @pl.when(core == 1)
    def _():
        arrived(14)

    b0, b1 = _block(me, 7, 0), _block(me, 7, 1)
    project(14, (b0,))

    def against(new, start, stop):
        def four(i, _):
            attend([both(new, _block(me, 2 * i + j, side)) for j in (0, 1) for side in (0, 1)])

        lax.fori_loop(start, stop, four, None)

    against(b0, 0, 1)

    @pl.when(core == 0)
    def _():
        half(15, 15, 1, 15, 16, partner).wait_recv()
        half(15, 15, 1, 15, 16, partner).start()

    against(b0, 1, 3)
    attend([both(b0, _block(me, 6, 0)), both(b0, _block(me, 6, 1)), (b0, b0, True)])

    def finish(b):
        rows = pl.ds(pl.multiple_of(b * BLK, BLK), BLK)
        for n in range(N):
            at = (b * N + n) * MR
            out = mix_s[pl.ds(pl.multiple_of(at, 8), HEAD), :] * (1 / mix_s[pl.ds(pl.multiple_of(at + HEAD, 8), 1), :])
            seen_s[rows, n * HEAD : (n + 1) * HEAD] = out.astype(jnp.bfloat16).T

    def piece(dev, r, count=PIECE):
        return seen_s.at[pl.ds(pl.multiple_of(dev * ROWS + r * PIECE, PIECE), count), :]

    def part(i, theirs, c, r, count=PIECE):
        return part_s.at[i, pl.ds(pl.multiple_of(r * PIECE, PIECE), count), pl.ds(pl.multiple_of((2 * theirs + c) * W, HEAD), W)]

    def across(i, r, c, chip):
        return pltpu.make_async_remote_copy(src_ref=piece(chip + c, r), dst_ref=part(i, 1, core, r), send_sem=send2.at[17 + 8 * i + 2 * r + c],
                                            recv_sem=recv2.at[10 + 8 * i + 2 * r + core], device_id={"tp": yn + c}, device_id_type=MESH)

    def across_wait(i, r):
        for c in (0, 1):
            pltpu.make_async_remote_copy(src_ref=part(i, 1, c, r), dst_ref=part(i, 1, c, r), send_sem=send2.at[0],
                                         recv_sem=recv2.at[10 + 8 * i + 2 * r + c], device_id={"tp": partner}, device_id_type=MESH).wait_recv()

    def own(j, c):
        i, r, count = ((0, 0, BLK), (0, 2, BLK), (1, 0, ROWS))[j]
        return piece((xn, xn, base)[j] + c, r, count), part(i, 0, core, r, count)

    def hand(j):
        src, dst = own(j, 1 - core)
        return pltpu.make_async_remote_copy(src_ref=src, dst_ref=dst, send_sem=send2.at[(33, 34, 51)[j]], recv_sem=recv2.at[(26, 27, 44)[j]],
                                            device_id={"tp": partner}, device_id_type=MESH)

    def keep(j):
        src, dst = own(j, core)
        return pltpu.make_async_copy(src, dst, lsem.at[j])

    def give_own(j):
        hand(j).start()
        keep(j).start()

    def have_own(j):
        keep(j).wait()
        hand(j).wait_recv()

    def give(q, r):
        at = (pl.ds(pl.multiple_of(r * PIECE, PIECE), PIECE), pl.ds(pl.multiple_of(q * WIDE, WIDE), WIDE))
        return pltpu.make_async_remote_copy(src_ref=a_s.at[at], dst_ref=sum_s.at[at], send_sem=send2.at[35 + 4 * q + r],
                                            recv_sem=recv2.at[28 + 4 * q + r], device_id={"tp": xn + core}, device_id_type=MESH)

    def partial_sum(q, r):
        rows, columns = pl.ds(pl.multiple_of(r * PIECE, PIECE), PIECE), pl.ds(pl.multiple_of(q * WIDE, WIDE), WIDE)
        a_s[rows, columns] = _dot(part_s[0, rows, :], wo_s[:, columns], 1, 0).astype(jnp.bfloat16)
        give(q, r).start()

    def far(half):
        for c in (0, 1):
            finish(2 * (dg + c) + half)
        for r in (2 * half, 2 * half + 1):
            for c in (0, 1):
                across(0, r, c, dg).start()

    far(0)
    @pl.when(core == 0)
    def _():
        half(15, 15, 0, 13, 15, partner).wait_recv()

    @pl.when(core == 1)
    def _():
        half(15, 15, 1, 15, 16, partner).wait_recv()

    project(15, (b1,))
    against(b1, 2, 3)
    for c in (0, 1):
        finish(2 * (xn + c))
    give_own(0)
    wo_in(0)
    wo_in(1)
    against(b1, 0, 1)
    for i in (*range(7), *range(8, 13)):
        remote(0, 0, i, partner).wait_send()

    @pl.when(core == 0)
    def _():
        for i in (7, 13):
            remote(0, 0, i, partner).wait_send()
        for i in (14, 15):
            half(0, 0, 0, i, 15, partner).wait_send()

    @pl.when(core == 1)
    def _():
        for i in (7, 13):
            half(0, 0, 0, i, 15, partner).wait_send()

    send_wo(1 - core, 1 - core, 0, 1 - core, partner).wait_recv()
    wo_all(0)
    wo_all(1)
    have_own(0)

    def early(r, _):
        across_wait(0, r)
        partial_sum(0, r)
        partial_sum(1, r)

    lax.fori_loop(0, 1, early, None)
    against(b1, 1, 2)
    attend([both(b1, _block(me, 6, 0)), both(b1, _block(me, 6, 1)), both(b1, b0), (b1, b1, True)])
    far(1)
    wo_out(2).start()
    wo_out(3).start()
    for c in (0, 1):
        finish(2 * (xn + c) + 1)
    give_own(1)
    lax.fori_loop(1, 2, early, None)
    for b in range(4):
        finish(2 * yn + b)
    for r in range(4):
        for c in (0, 1):
            across(1, r, c, yn).start()
    for b in range(4):
        finish(2 * base + b)
    give_own(2)
    have_own(1)
    lax.fori_loop(2, 4, early, None)
    have_own(2)

    def ours(n, _):
        out = _dot(part_s[1, :, : 2 * W], wo_s[: 2 * W, pl.ds(pl.multiple_of(n * BLK, BLK), BLK)], 1, 0)
        mix_s[pl.ds(pl.multiple_of(n * ROWS, ROWS), ROWS), :] = out

    lax.fori_loop(0, D // BLK, ours, None)
    for q in (2, 3):
        wo_in(q)
        wo_all(q)

        def late(r, _):
            partial_sum(q, r)

        lax.fori_loop(0, 4, late, None)

    def last(r, _):
        rows = pl.ds(pl.multiple_of(r * PIECE, PIECE), PIECE)
        across_wait(1, r)
        for n in range(D // BLK):
            at = pl.ds(pl.multiple_of(n * ROWS + r * PIECE, PIECE), PIECE)
            mix_s[at, :] += _dot(part_s[1, rows, 2 * W :], wo_s[2 * W :, n * BLK : (n + 1) * BLK], 1, 0)
        for q in range(4):
            give(q, r).wait_recv()
        for n in range(D // BLK):
            at = slice(n * BLK, (n + 1) * BLK)
            total = mix_s[pl.ds(pl.multiple_of(n * ROWS + r * PIECE, PIECE), PIECE), :] + sum_s[rows, at].astype(jnp.float32)
            y_ref[rows, at] = (x_ref[rows, at].astype(jnp.float32) + total).astype(jnp.bfloat16)

    lax.fori_loop(0, 4, last, None)

    send_wo(core, core, 0, core, partner).wait_send()

    for q in range(4):
        wo_out(q).wait_send()
        wo_on(q).wait_send()

    def sent(r, _):
        for c in (0, 1):
            across(0, r, c, dg).wait_send()
            across(1, r, c, yn).wait_send()
        for q in range(4):
            give(q, r).wait_send()

    lax.fori_loop(0, 4, sent, None)
    for j in range(3):
        hand(j).wait_send()


def solution(mesh):
    def step(x, gain, wq, wk, wv, wo):
        lo, hi = _rope_tables()
        any_space = pl.BlockSpec(memory_space=pl.ANY)
        vmem = pl.BlockSpec(memory_space=pltpu.VMEM)
        return pl.pallas_call(
            kernel,
            out_shape=pltpu.VMEM((ROWS, D), jnp.bfloat16),
            in_specs=[any_space, vmem, any_space, any_space, any_space, any_space, any_space, vmem],
            out_specs=vmem,
            scratch_shapes=[
                pltpu.VMEM((ROWS, D), jnp.bfloat16),
                pltpu.VMEM((2, BLK, HEAD), jnp.float32),
                pltpu.VMEM((NBLK * BLK, D), jnp.bfloat16),
                pltpu.VMEM((D, 3 * W), jnp.bfloat16),
                pltpu.VMEM((NBLK, N, BLK, HEAD), jnp.bfloat16),
                pltpu.VMEM((NBLK, N, BLK, HEAD), jnp.bfloat16),
                pltpu.VMEM((NBLK, N, VR, BLK), jnp.bfloat16),
                pltpu.VMEM((NBLK, 8, BLK), jnp.float32),
                pltpu.VMEM((NBLK * N * MR, BLK), jnp.float32),
                pltpu.VMEM((4 * W, D), jnp.bfloat16),
                pltpu.VMEM((NBLK * BLK, W), jnp.bfloat16),
                pltpu.VMEM((2, ROWS, 4 * W), jnp.bfloat16),
                pltpu.VMEM((ROWS, D), jnp.bfloat16),
                pltpu.SemaphoreType.DMA((7,)),
                pltpu.SemaphoreType.DMA((16,)),
                pltpu.SemaphoreType.DMA((17,)),
                pltpu.SemaphoreType.DMA((52,)),
                pltpu.SemaphoreType.DMA((45,)),
                pltpu.SemaphoreType.DMA((3,)),
            ],
            compiler_params=pltpu.CompilerParams(collective_id=0, has_side_effects=True, vmem_limit_bytes=61 * 2**20),
            cost_estimate=pl.CostEstimate(flops=40 * 10**9, bytes_accessed=10**7, transcendentals=3 * 10**7),
        )(x, gain, wq, wk, wv, wo, jnp.asarray(lo), jnp.asarray(hi))

    tokens, columns = P(("dp", "tp"), None), P(None, "tp")
    return jax.shard_map(
        step,
        mesh=mesh,
        in_specs=(tokens, P(None), columns, columns, columns, P("tp", None)),
        out_specs=tokens,
        check_vma=False,
    )
```

```python
import functools

import jax
import jax.numpy as jnp
import numpy as np
from jax import lax
from jax.experimental import pallas as pl
from jax.experimental.pallas import tpu as pltpu
from jax.sharding import PartitionSpec as P

MESH = pl.DeviceIdType.MESH
NEG = -1e30
HIDDEN = 2 * NEG
LOG2E = 1.4426950408889634
HEAD = 128
THETA = 10000
WIDE = 512
PIECE = 128
AHEAD = 4
N = 3
BLK = 256
ROWS = 512
NBLK = 16
D = 2048
W = N * HEAD
VR = 144
MR = HEAD + 8


def _dot(a, b, ca, cb):
    return lax.dot_general(a, b, (((ca,), (cb,)), ((), ())), preferred_element_type=jnp.float32)


def _rope_tables():
    half = HEAD // 2
    freq = THETA ** (-np.arange(half, dtype=np.float64) / half)
    sign = np.concatenate([-np.ones(half), np.ones(half)])
    def table(pos):
        ang = pos[:, None] * np.concatenate([freq, freq])
        return np.cos(ang).astype(np.float32), (np.sin(ang) * sign).astype(np.float32)
    lo = np.stack(table(np.arange(BLK, dtype=np.float64)))
    hi = np.stack(table(np.arange(NBLK, dtype=np.float64) * BLK))
    return lo, hi


def _place(me):
    core = me % 2
    y = (me // 2) % 2
    x = me // 4
    base = me - core
    xn = base + 4 - 8 * x
    yn = base + 2 - 4 * y
    dg = xn + 2 - 4 * y
    return core, base, xn, yn, dg


def _block(me, k, side):
    core, base, xn, yn, dg = _place(me)
    odd = k % 2
    flip = side + odd - 2 * side * odd
    near = jnp.where(side == 0, xn, yn) if not isinstance(side, int) else (xn if side == 0 else yn)
    dev = jnp.where(k < 1, me, jnp.where(k < 2, me + 1 - 2 * core, jnp.where(k < 6, near + flip, dg + 1 - flip)))
    half = jnp.where((k == 2) | (k == 3), 1 - side, side)
    return 2 * dev + half


def kernel(x_hbm, gain_ref, wq_ref, wk_ref, wv_ref, wo_ref, lo_hbm, hi_ref, y_ref,
           x_ref, lo_ref, a_s, w_s, q_s, k_s, v_s, top_s, mix_s, wo_s, seen_s, part_s, sum_s, wsem, send, recv, send2, recv2, lsem):
    me = lax.axis_index("tp")
    core, base, xn, yn, dg = _place(me)
    partner = base + 1 - core
    link = jnp.where(core == 0, xn, yn + 1)
    first = 1 - core

    def fetch(half, sem):
        rows = pl.ds(pl.multiple_of(half * BLK, BLK), BLK)
        return pltpu.make_async_copy(x_hbm.at[rows, :], x_ref.at[rows, :], wsem.at[sem])

    fetch(first, 4).start()
    fetch(1 - first, 5).start()

    barrier = pltpu.get_barrier_semaphore()
    for other in (partner, xn + core, yn, yn + 1):
        pl.semaphore_signal(barrier, inc=1, device_id={"tp": other}, device_id_type=MESH)

    loads = [pltpu.make_async_copy(w, w_s.at[:, pl.ds(i * W, W)], wsem.at[i]) for i, w in enumerate((wq_ref, wk_ref, wv_ref))]
    loads.append(pltpu.make_async_copy(lo_hbm, lo_ref, wsem.at[6]))
    for c in loads:
        c.start()
    wo_mine = wo_s.at[pl.ds(pl.multiple_of(core * W, W), W), :]
    wo_load = pltpu.make_async_copy(wo_ref, wo_mine, wsem.at[3])
    wo_load.start()

    def slot(s):
        return a_s.at[pl.ds(pl.multiple_of(s * BLK, BLK), BLK), :]

    def remote(src, dst, sem, dev):
        return pltpu.make_async_remote_copy(src_ref=slot(src), dst_ref=slot(dst), send_sem=send.at[sem], recv_sem=recv.at[dst],
                                            device_id={"tp": dev}, device_id_type=MESH)

    def send_wo(src, dst, sem, arrival, dev, q=None):
        columns = slice(None) if q is None else pl.ds(pl.multiple_of(q * WIDE, WIDE), WIDE)
        at = lambda i: wo_s.at[pl.ds(pl.multiple_of(i * W, W), W), columns]
        return pltpu.make_async_remote_copy(src_ref=at(src), dst_ref=at(dst), send_sem=send2.at[sem], recv_sem=recv2.at[arrival],
                                            device_id={"tp": dev}, device_id_type=MESH)

    def wo_out(q):
        return send_wo(core, 2 + core, 1 + q, 2 + 2 * q + core, yn + core, q)

    def wo_on(q):
        return send_wo(2 + core, 2 + core, 5 + q, 2 + 2 * q + core, partner, q)

    def wo_in(q):
        send_wo(2 + core, 2 + core, 0, 2 + 2 * q + core, partner, q).wait_recv()
        wo_on(q).start()

    def wo_all(q):
        send_wo(3 - core, 3 - core, 0, 3 + 2 * q - core, partner, q).wait_recv()

    def half(src, dst, h, sem, arrival, dev):
        at = lambda i: a_s.at[pl.ds(pl.multiple_of(i * BLK + h * PIECE, PIECE), PIECE), :]
        return pltpu.make_async_remote_copy(src_ref=at(src), dst_ref=at(dst), send_sem=send.at[sem], recv_sem=recv.at[arrival],
                                            device_id={"tp": dev}, device_id_type=MESH)

    def arrived(s):
        return pltpu.make_async_remote_copy(src_ref=slot(s), dst_ref=slot(s), send_sem=send.at[0], recv_sem=recv.at[s],
                                            device_id={"tp": partner}, device_id_type=MESH).wait_recv()

    gain = gain_ref[...].astype(jnp.float32).reshape(1, D)

    def norm(start, count):
        def rows(i, _):
            at = pl.ds(pl.multiple_of(start + i * 16, 16), 16)
            wide = x_ref[at, :].astype(jnp.float32)
            scale = lax.rsqrt(jnp.mean(wide * wide, -1, keepdims=True) + 1e-6)
            a_s[at, :] = (wide * scale * gain).astype(jnp.bfloat16)
        lax.fori_loop(0, count // 16, rows, None, unroll=8 if count == 256 else 2)

    fetch(first, 4).wait()
    norm(first * BLK, BLK)
    fetch(1 - first, 5).wait()
    pl.semaphore_wait(barrier, 4)
    norm((1 - first) * BLK, 32)
    remote(first, 4 + core, 2, link).start()
    remote(first, 2 + first, 0, partner).start()
    norm((1 - first) * BLK + 32, BLK - 32)
    v_s[:, :, HEAD:, :] = jnp.ones((NBLK, N, VR - HEAD, BLK), jnp.bfloat16)
    top_s[...] = jnp.full(top_s.shape, NEG, jnp.float32)

    def clear(i, _):
        mix_s[pl.ds(pl.multiple_of(i * MR, MR), MR), :] = jnp.zeros((MR, BLK), jnp.float32)

    lax.fori_loop(0, NBLK * N, clear, None)
    remote(1 - first, 3 - first, 1, partner).start()
    for c in loads:
        c.wait()
    wo_load.wait()
    send_wo(core, core, 0, core, partner).start()

    scale_e = HEAD ** -0.5 * LOG2E

    def project(first_slot, blocks):
        here = pl.ds(pl.multiple_of(first_slot * BLK, BLK), BLK * len(blocks))
        tables = []
        for b in blocks:
            ch, sh = hi_ref[0, pl.ds(b, 1), :], hi_ref[1, pl.ds(b, 1), :]
            cl, sl = lo_ref[0], lo_ref[1]
            tables.append((ch * cl - sh * sl, sh * cl + ch * sl))
        for g in range(0, 3 * N, 2):
            width = min(2, 3 * N - g) * HEAD
            out = _dot(a_s[here, :], w_s[:, g * HEAD : g * HEAD + width], 1, 0).astype(jnp.bfloat16)
            for i in range(width // HEAD):
                kind, n = divmod(g + i, N)
                for b, block in enumerate(blocks):
                    t = out[b * BLK : (b + 1) * BLK, i * HEAD : (i + 1) * HEAD]
                    if kind == 2:
                        v_s[block, n, :HEAD, :] = t.T
                    else:
                        t = t.astype(jnp.float32)
                        t = t * tables[b][0] + pltpu.roll(t, HEAD // 2, 1) * tables[b][1]
                        (q_s if kind == 0 else k_s)[block, n] = t.astype(jnp.bfloat16)

    def attend(pairs):
        strips = [(q, k, masked, n) for q, k, masked in pairs for n in range(N)]
        if any(masked for _, _, masked in pairs):
            ok = lax.broadcasted_iota(jnp.int32, (BLK, BLK), 1) >= lax.broadcasted_iota(jnp.int32, (BLK, BLK), 0)

        def score(q, k, masked, n):
            return _dot(k_s[k, n], q_s[q, n], 1, 1)

        ahead = [score(*strip) for strip in strips[:AHEAD]]
        for i, (q, k, masked, n) in enumerate(strips):
            if i + AHEAD < len(strips):
                ahead.append(score(*strips[i + AHEAD]))
            s = ahead.pop(0)
            if masked:
                s = jnp.where(ok, s, HIDDEN)
            old = top_s[q, n : n + 1, :]
            top = jnp.maximum(old, s.max(axis=0, keepdims=True))
            top_s[q, n : n + 1, :] = top
            p = jnp.exp2((s - top) * scale_e).astype(jnp.bfloat16)
            keep = jnp.exp2((old - top) * scale_e)
            mix = pl.ds(pl.multiple_of((q * N + n) * MR, 8), MR)
            mix_s[mix, :] = mix_s[mix, :] * keep + _dot(v_s[k, n], p, 1, 0)[:MR, :]

    def both(new, old):
        return jnp.maximum(new, old), jnp.minimum(new, old), False

    def event(k, _):
        b0, b1 = _block(me, k, 0), _block(me, k, 1)

        @pl.when(k >= 2)
        def _():
            arrived(2 * k + 1 - core)

            @pl.when((k == 2) | ((k == 3) & (core == 0)))
            def _():
                remote(2 * k + 1 - core, 2 * k + 8 + core, 4 + k, link).start()

            @pl.when((k == 4) & (core == 0))
            def _():
                half(9, 15, 0, 16, 15, link).start()
                half(9, 15, 1, 14, 16, link).start()

            @pl.when((k == 3) & (core == 1))
            def _():
                wo_out(0).start()
                wo_out(1).start()
                wo_out(2).start()

        project(2 * k, (b0, b1))

        @pl.when(k == 0)
        def _():
            arrived(2 + first)
            remote(2 + first, 6 + core, 3, link).start()
            remote(1 - first, 8 + core, 4, link).start()
            arrived(3 - first)
            remote(3 - first, 10 + core, 5, link).start()

        def older(j, _):
            pairs = []
            for new in (b0, b1):
                for side in (0, 1):
                    pairs.append(both(new, _block(me, j, side)))
            attend(pairs)

        @pl.when((k == 6) & (core == 0))
        def _():
            wo_out(0).start()
            wo_out(1).start()
            wo_out(2).start()

        lax.fori_loop(0, k, older, None)

        @pl.when((k >= 1) & ((k < 6) | (core == 0)))
        def _():
            arrived(2 * k + 2 + core)
            remote(2 * k + 2 + core, 2 * k + 2 + core, 7 + k, partner).start()


        attend([both(b0, b1), (b0, b0, True), (b1, b1, True)])

    lax.fori_loop(0, 7, event, None)

    @pl.when(core == 1)
    def _():
        arrived(14)

    b0, b1 = _block(me, 7, 0), _block(me, 7, 1)
    project(14, (b0,))

    def against(new, start, stop):
        def four(i, _):
            attend([both(new, _block(me, 2 * i + j, side)) for j in (0, 1) for side in (0, 1)])

        lax.fori_loop(start, stop, four, None)

    against(b0, 0, 2)

    @pl.when(core == 0)
    def _():
        half(15, 15, 0, 17, 15, partner).wait_recv()
        half(15, 15, 0, 17, 15, partner).start()

    against(b0, 2, 3)
    attend([both(b0, _block(me, 6, 0)), both(b0, _block(me, 6, 1)), (b0, b0, True)])

    def finish(b):
        rows = pl.ds(pl.multiple_of(b * BLK, BLK), BLK)
        for n in range(N):
            at = (b * N + n) * MR
            out = mix_s[pl.ds(pl.multiple_of(at, 8), HEAD), :] * (1 / mix_s[pl.ds(pl.multiple_of(at + HEAD, 8), 1), :])
            seen_s[rows, n * HEAD : (n + 1) * HEAD] = out.astype(jnp.bfloat16).T

    def piece(dev, r, count=PIECE):
        return seen_s.at[pl.ds(pl.multiple_of(dev * ROWS + r * PIECE, PIECE), count), :]

    def part(i, theirs, c, r, count=PIECE):
        return part_s.at[i, pl.ds(pl.multiple_of(r * PIECE, PIECE), count), pl.ds(pl.multiple_of((2 * theirs + c) * W, HEAD), W)]

    def across(i, r, c, chip):
        return pltpu.make_async_remote_copy(src_ref=piece(chip + c, r), dst_ref=part(i, 1, core, r), send_sem=send2.at[17 + 8 * i + 2 * r + c],
                                            recv_sem=recv2.at[10 + 8 * i + 2 * r + core], device_id={"tp": yn + c}, device_id_type=MESH)

    def across_wait(i, r):
        for c in (0, 1):
            pltpu.make_async_remote_copy(src_ref=part(i, 1, c, r), dst_ref=part(i, 1, c, r), send_sem=send2.at[0],
                                         recv_sem=recv2.at[10 + 8 * i + 2 * r + c], device_id={"tp": partner}, device_id_type=MESH).wait_recv()

    def own(j, c):
        i, r, count = ((0, 0, BLK), (0, 2, BLK), (1, 0, ROWS))[j]
        return piece((xn, xn, base)[j] + c, r, count), part(i, 0, core, r, count)

    def hand(j):
        src, dst = own(j, 1 - core)
        return pltpu.make_async_remote_copy(src_ref=src, dst_ref=dst, send_sem=send2.at[(33, 34, 51)[j]], recv_sem=recv2.at[(26, 27, 44)[j]],
                                            device_id={"tp": partner}, device_id_type=MESH)

    def keep(j):
        src, dst = own(j, core)
        return pltpu.make_async_copy(src, dst, lsem.at[j])

    def give_own(j):
        hand(j).start()
        keep(j).start()

    def have_own(j):
        keep(j).wait()
        hand(j).wait_recv()

    def give(q, r):
        at = (pl.ds(pl.multiple_of(r * PIECE, PIECE), PIECE), pl.ds(pl.multiple_of(q * WIDE, WIDE), WIDE))
        return pltpu.make_async_remote_copy(src_ref=a_s.at[at], dst_ref=sum_s.at[at], send_sem=send2.at[35 + 4 * q + r],
                                            recv_sem=recv2.at[28 + 4 * q + r], device_id={"tp": xn + core}, device_id_type=MESH)

    def partial_sum(q, r):
        rows, columns = pl.ds(pl.multiple_of(r * PIECE, PIECE), PIECE), pl.ds(pl.multiple_of(q * WIDE, WIDE), WIDE)
        a_s[rows, columns] = _dot(part_s[0, rows, :], wo_s[:, columns], 1, 0).astype(jnp.bfloat16)
        give(q, r).start()

    def far(half):
        for c in (0, 1):
            finish(2 * (dg + c) + half)
        for r in (2 * half, 2 * half + 1):
            for c in (0, 1):
                across(0, r, c, dg).start()

    far(0)
    wo_in(0)
    wo_in(1)
    @pl.when(core == 0)
    def _():
        half(15, 15, 1, 15, 16, partner).wait_recv()
        half(15, 15, 1, 15, 16, partner).start()

    @pl.when(core == 1)
    def _():
        half(15, 15, 0, 17, 15, partner).wait_recv()
        half(15, 15, 1, 15, 16, partner).wait_recv()

    project(15, (b1,))
    attend([both(b1, _block(me, 4, 0)), both(b1, _block(me, 5, 0))])
    for c in (0, 1):
        finish(2 * (xn + c))
    give_own(0)
    attend([both(b1, _block(me, 4, 1)), both(b1, _block(me, 5, 1))])
    for i in (*range(7), *range(8, 13)):
        remote(0, 0, i, partner).wait_send()

    @pl.when(core == 0)
    def _():
        for i in (7, 13):
            remote(0, 0, i, partner).wait_send()
        for i in (14, 15, 16, 17):
            half(0, 0, 0, i, 15, partner).wait_send()

    send_wo(1 - core, 1 - core, 0, 1 - core, partner).wait_recv()
    wo_all(0)
    wo_all(1)
    have_own(0)

    def early(r, _):
        across_wait(0, r)
        partial_sum(0, r)
        partial_sum(1, r)

    lax.fori_loop(0, 1, early, None)
    against(b1, 0, 2)
    attend([both(b1, _block(me, 6, 0)), both(b1, _block(me, 6, 1)), both(b1, b0), (b1, b1, True)])
    far(1)
    wo_out(3).start()
    for c in (0, 1):
        finish(2 * (xn + c) + 1)
    give_own(1)
    lax.fori_loop(1, 2, early, None)
    for b in range(4):
        finish(2 * yn + b)
    for r in range(4):
        for c in (0, 1):
            across(1, r, c, yn).start()
    for b in range(4):
        finish(2 * base + b)
    give_own(2)
    have_own(1)
    lax.fori_loop(2, 4, early, None)
    have_own(2)

    def ours(n, _):
        out = _dot(part_s[1, :, : 2 * W], wo_s[: 2 * W, pl.ds(pl.multiple_of(n * BLK, BLK), BLK)], 1, 0)
        mix_s[pl.ds(pl.multiple_of(n * ROWS, ROWS), ROWS), :] = out

    lax.fori_loop(0, D // BLK, ours, None)
    for q in (2, 3):
        wo_in(q)
        wo_all(q)

        def late(r, _):
            partial_sum(q, r)

        lax.fori_loop(0, 4, late, None)

    def last(r, _):
        rows = pl.ds(pl.multiple_of(r * PIECE, PIECE), PIECE)
        across_wait(1, r)
        for n in range(D // BLK):
            at = pl.ds(pl.multiple_of(n * ROWS + r * PIECE, PIECE), PIECE)
            mix_s[at, :] += _dot(part_s[1, rows, 2 * W :], wo_s[2 * W :, n * BLK : (n + 1) * BLK], 1, 0)
        for q in range(4):
            give(q, r).wait_recv()
        for n in range(D // BLK):
            at = slice(n * BLK, (n + 1) * BLK)
            total = mix_s[pl.ds(pl.multiple_of(n * ROWS + r * PIECE, PIECE), PIECE), :] + sum_s[rows, at].astype(jnp.float32)
            y_ref[rows, at] = (x_ref[rows, at].astype(jnp.float32) + total).astype(jnp.bfloat16)

    lax.fori_loop(0, 4, last, None)

    send_wo(core, core, 0, core, partner).wait_send()

    for q in range(4):
        wo_out(q).wait_send()
        wo_on(q).wait_send()

    def sent(r, _):
        for c in (0, 1):
            across(0, r, c, dg).wait_send()
            across(1, r, c, yn).wait_send()
        for q in range(4):
            give(q, r).wait_send()

    lax.fori_loop(0, 4, sent, None)
    for j in range(3):
        hand(j).wait_send()


def solution(mesh):
    def step(x, gain, wq, wk, wv, wo):
        lo, hi = _rope_tables()
        any_space = pl.BlockSpec(memory_space=pl.ANY)
        vmem = pl.BlockSpec(memory_space=pltpu.VMEM)
        return pl.pallas_call(
            kernel,
            out_shape=pltpu.VMEM((ROWS, D), jnp.bfloat16),
            in_specs=[any_space, vmem, any_space, any_space, any_space, any_space, any_space, vmem],
            out_specs=vmem,
            scratch_shapes=[
                pltpu.VMEM((ROWS, D), jnp.bfloat16),
                pltpu.VMEM((2, BLK, HEAD), jnp.float32),
                pltpu.VMEM((NBLK * BLK, D), jnp.bfloat16),
                pltpu.VMEM((D, 3 * W), jnp.bfloat16),
                pltpu.VMEM((NBLK, N, BLK, HEAD), jnp.bfloat16),
                pltpu.VMEM((NBLK, N, BLK, HEAD), jnp.bfloat16),
                pltpu.VMEM((NBLK, N, VR, BLK), jnp.bfloat16),
                pltpu.VMEM((NBLK, 8, BLK), jnp.float32),
                pltpu.VMEM((NBLK * N * MR, BLK), jnp.float32),
                pltpu.VMEM((4 * W, D), jnp.bfloat16),
                pltpu.VMEM((NBLK * BLK, W), jnp.bfloat16),
                pltpu.VMEM((2, ROWS, 4 * W), jnp.bfloat16),
                pltpu.VMEM((ROWS, D), jnp.bfloat16),
                pltpu.SemaphoreType.DMA((7,)),
                pltpu.SemaphoreType.DMA((18,)),
                pltpu.SemaphoreType.DMA((17,)),
                pltpu.SemaphoreType.DMA((52,)),
                pltpu.SemaphoreType.DMA((45,)),
                pltpu.SemaphoreType.DMA((3,)),
            ],
            compiler_params=pltpu.CompilerParams(collective_id=0, has_side_effects=True, vmem_limit_bytes=61 * 2**20),
            cost_estimate=pl.CostEstimate(flops=40 * 10**9, bytes_accessed=10**7, transcendentals=3 * 10**7),
        )(x, gain, wq, wk, wv, wo, jnp.asarray(lo), jnp.asarray(hi))

    tokens, columns = P(("dp", "tp"), None), P(None, "tp")
    return jax.shard_map(
        step,
        mesh=mesh,
        in_specs=(tokens, P(None), columns, columns, columns, P("tp", None)),
        out_specs=tokens,
        check_vma=False,
    )
```

```python
import functools

import jax
import jax.numpy as jnp
import numpy as np
from jax import lax
from jax.experimental import pallas as pl
from jax.experimental.pallas import tpu as pltpu
from jax.sharding import PartitionSpec as P

MESH = pl.DeviceIdType.MESH
NEG = -1e30
HIDDEN = 2 * NEG
LOG2E = 1.4426950408889634
HEAD = 128
THETA = 10000
WIDE = 512
PIECE = 128
AHEAD = 6
N = 3
BLK = 256
ROWS = 512
NBLK = 16
D = 2048
W = N * HEAD
VR = 144
MR = HEAD + 8


def _dot(a, b, ca, cb):
    return lax.dot_general(a, b, (((ca,), (cb,)), ((), ())), preferred_element_type=jnp.float32)


def _rope_tables():
    half = HEAD // 2
    freq = THETA ** (-np.arange(half, dtype=np.float64) / half)
    sign = np.concatenate([-np.ones(half), np.ones(half)])
    def table(pos):
        ang = pos[:, None] * np.concatenate([freq, freq])
        return np.cos(ang).astype(np.float32), (np.sin(ang) * sign).astype(np.float32)
    lo = np.stack(table(np.arange(BLK, dtype=np.float64)))
    hi = np.stack(table(np.arange(NBLK, dtype=np.float64) * BLK))
    return lo, hi


def _place(me):
    core = me % 2
    y = (me // 2) % 2
    x = me // 4
    base = me - core
    xn = base + 4 - 8 * x
    yn = base + 2 - 4 * y
    dg = xn + 2 - 4 * y
    return core, base, xn, yn, dg


def _block(me, k, side):
    core, base, xn, yn, dg = _place(me)
    odd = k % 2
    flip = side + odd - 2 * side * odd
    near = jnp.where(side == 0, xn, yn) if not isinstance(side, int) else (xn if side == 0 else yn)
    dev = jnp.where(k < 1, me, jnp.where(k < 2, me + 1 - 2 * core, jnp.where(k < 6, near + flip, dg + 1 - flip)))
    half = jnp.where((k == 2) | (k == 3), 1 - side, side)
    return 2 * dev + half


def kernel(x_hbm, gain_ref, wq_ref, wk_ref, wv_ref, wo_ref, lo_hbm, hi_ref, y_ref,
           x_ref, lo_ref, a_s, w_s, q_s, k_s, v_s, top_s, mix_s, wo_s, seen_s, part_s, sum_s, wsem, send, recv, send2, recv2, lsem):
    me = lax.axis_index("tp")
    core, base, xn, yn, dg = _place(me)
    partner = base + 1 - core
    link = jnp.where(core == 0, xn, yn + 1)
    first = 1 - core

    def fetch(half, sem):
        rows = pl.ds(pl.multiple_of(half * BLK, BLK), BLK)
        return pltpu.make_async_copy(x_hbm.at[rows, :], x_ref.at[rows, :], wsem.at[sem])

    fetch(first, 4).start()
    fetch(1 - first, 5).start()

    barrier = pltpu.get_barrier_semaphore()
    for other in (partner, xn + core, yn, yn + 1):
        pl.semaphore_signal(barrier, inc=1, device_id={"tp": other}, device_id_type=MESH)

    loads = [pltpu.make_async_copy(w, w_s.at[:, pl.ds(i * W, W)], wsem.at[i]) for i, w in enumerate((wq_ref, wk_ref, wv_ref))]
    loads.append(pltpu.make_async_copy(lo_hbm, lo_ref, wsem.at[6]))
    for c in loads:
        c.start()
    wo_mine = wo_s.at[pl.ds(pl.multiple_of(core * W, W), W), :]
    wo_load = pltpu.make_async_copy(wo_ref, wo_mine, wsem.at[3])
    wo_load.start()

    def slot(s):
        return a_s.at[pl.ds(pl.multiple_of(s * BLK, BLK), BLK), :]

    def remote(src, dst, sem, dev):
        return pltpu.make_async_remote_copy(src_ref=slot(src), dst_ref=slot(dst), send_sem=send.at[sem], recv_sem=recv.at[dst],
                                            device_id={"tp": dev}, device_id_type=MESH)

    def send_wo(src, dst, sem, arrival, dev, q=None):
        columns = slice(None) if q is None else pl.ds(pl.multiple_of(q * WIDE, WIDE), WIDE)
        at = lambda i: wo_s.at[pl.ds(pl.multiple_of(i * W, W), W), columns]
        return pltpu.make_async_remote_copy(src_ref=at(src), dst_ref=at(dst), send_sem=send2.at[sem], recv_sem=recv2.at[arrival],
                                            device_id={"tp": dev}, device_id_type=MESH)

    def wo_out(q):
        return send_wo(core, 2 + core, 1 + q, 2 + 2 * q + core, yn + core, q)

    def wo_on(q):
        return send_wo(2 + core, 2 + core, 5 + q, 2 + 2 * q + core, partner, q)

    def wo_in(q):
        send_wo(2 + core, 2 + core, 0, 2 + 2 * q + core, partner, q).wait_recv()
        wo_on(q).start()

    def wo_all(q):
        send_wo(3 - core, 3 - core, 0, 3 + 2 * q - core, partner, q).wait_recv()

    def half(src, dst, h, sem, arrival, dev):
        at = lambda i: a_s.at[pl.ds(pl.multiple_of(i * BLK + h * PIECE, PIECE), PIECE), :]
        return pltpu.make_async_remote_copy(src_ref=at(src), dst_ref=at(dst), send_sem=send.at[sem], recv_sem=recv.at[arrival],
                                            device_id={"tp": dev}, device_id_type=MESH)

    def arrived(s):
        return pltpu.make_async_remote_copy(src_ref=slot(s), dst_ref=slot(s), send_sem=send.at[0], recv_sem=recv.at[s],
                                            device_id={"tp": partner}, device_id_type=MESH).wait_recv()

    gain = gain_ref[...].astype(jnp.float32).reshape(1, D)

    def norm(start, count):
        def rows(i, _):
            at = pl.ds(pl.multiple_of(start + i * 16, 16), 16)
            wide = x_ref[at, :].astype(jnp.float32)
            scale = lax.rsqrt(jnp.mean(wide * wide, -1, keepdims=True) + 1e-6)
            a_s[at, :] = (wide * scale * gain).astype(jnp.bfloat16)
        lax.fori_loop(0, count // 16, rows, None, unroll=8 if count == 256 else 2)

    fetch(first, 4).wait()
    norm(first * BLK, BLK)
    fetch(1 - first, 5).wait()
    pl.semaphore_wait(barrier, 4)
    norm((1 - first) * BLK, 32)
    remote(first, 4 + core, 2, link).start()
    remote(first, 2 + first, 0, partner).start()
    norm((1 - first) * BLK + 32, BLK - 32)
    v_s[:, :, HEAD:, :] = jnp.ones((NBLK, N, VR - HEAD, BLK), jnp.bfloat16)
    top_s[...] = jnp.full(top_s.shape, NEG, jnp.float32)

    def clear(i, _):
        mix_s[pl.ds(pl.multiple_of(i * MR, MR), MR), :] = jnp.zeros((MR, BLK), jnp.float32)

    lax.fori_loop(0, NBLK * N, clear, None)
    remote(1 - first, 3 - first, 1, partner).start()
    for c in loads:
        c.wait()
    wo_load.wait()
    send_wo(core, core, 0, core, partner).start()

    scale_e = HEAD ** -0.5 * LOG2E

    def project(first_slot, blocks):
        here = pl.ds(pl.multiple_of(first_slot * BLK, BLK), BLK * len(blocks))
        tables = []
        for b in blocks:
            ch, sh = hi_ref[0, pl.ds(b, 1), :], hi_ref[1, pl.ds(b, 1), :]
            cl, sl = lo_ref[0], lo_ref[1]
            tables.append((ch * cl - sh * sl, sh * cl + ch * sl))
        for g in range(0, 3 * N, 2):
            width = min(2, 3 * N - g) * HEAD
            out = _dot(a_s[here, :], w_s[:, g * HEAD : g * HEAD + width], 1, 0).astype(jnp.bfloat16)
            for i in range(width // HEAD):
                kind, n = divmod(g + i, N)
                for b, block in enumerate(blocks):
                    t = out[b * BLK : (b + 1) * BLK, i * HEAD : (i + 1) * HEAD]
                    if kind == 2:
                        v_s[block, n, :HEAD, :] = t.T
                    else:
                        t = t.astype(jnp.float32)
                        t = t * tables[b][0] + pltpu.roll(t, HEAD // 2, 1) * tables[b][1]
                        (q_s if kind == 0 else k_s)[block, n] = t.astype(jnp.bfloat16)

    def attend(pairs):
        strips = [(q, k, masked, n) for q, k, masked in pairs for n in range(N)]
        if any(masked for _, _, masked in pairs):
            ok = lax.broadcasted_iota(jnp.int32, (BLK, BLK), 1) >= lax.broadcasted_iota(jnp.int32, (BLK, BLK), 0)

        def score(q, k, masked, n):
            return _dot(k_s[k, n], q_s[q, n], 1, 1)

        ahead = [score(*strip) for strip in strips[:AHEAD]]
        for i, (q, k, masked, n) in enumerate(strips):
            if i + AHEAD < len(strips):
                ahead.append(score(*strips[i + AHEAD]))
            s = ahead.pop(0)
            if masked:
                s = jnp.where(ok, s, HIDDEN)
            old = top_s[q, n : n + 1, :]
            top = jnp.maximum(old, s.max(axis=0, keepdims=True))
            top_s[q, n : n + 1, :] = top
            p = jnp.exp2((s - top) * scale_e).astype(jnp.bfloat16)
            keep = jnp.exp2((old - top) * scale_e)
            mix = pl.ds(pl.multiple_of((q * N + n) * MR, 8), MR)
            mix_s[mix, :] = mix_s[mix, :] * keep + _dot(v_s[k, n], p, 1, 0)[:MR, :]

    def both(new, old):
        return jnp.maximum(new, old), jnp.minimum(new, old), False

    def event(k, _):
        b0, b1 = _block(me, k, 0), _block(me, k, 1)

        @pl.when(k >= 2)
        def _():
            arrived(2 * k + 1 - core)

            @pl.when((k == 2) | ((k == 3) & (core == 0)))
            def _():
                remote(2 * k + 1 - core, 2 * k + 8 + core, 4 + k, link).start()

            @pl.when((k == 4) & (core == 0))
            def _():
                half(9, 15, 0, 16, 15, link).start()
                half(9, 15, 1, 14, 16, link).start()

            @pl.when((k == 3) & (core == 1))
            def _():
                wo_out(0).start()
                wo_out(1).start()
                wo_out(2).start()

        project(2 * k, (b0, b1))

        @pl.when(k == 0)
        def _():
            arrived(2 + first)
            remote(2 + first, 6 + core, 3, link).start()
            remote(1 - first, 8 + core, 4, link).start()
            arrived(3 - first)
            remote(3 - first, 10 + core, 5, link).start()

        def older(j, _):
            pairs = []
            for new in (b0, b1):
                for side in (0, 1):
                    pairs.append(both(new, _block(me, j, side)))
            attend(pairs)

        @pl.when((k == 6) & (core == 0))
        def _():
            wo_out(0).start()
            wo_out(1).start()
            wo_out(2).start()

        lax.fori_loop(0, k, older, None)

        @pl.when((k >= 1) & ((k < 6) | (core == 0)))
        def _():
            arrived(2 * k + 2 + core)
            remote(2 * k + 2 + core, 2 * k + 2 + core, 7 + k, partner).start()


        attend([both(b0, b1), (b0, b0, True), (b1, b1, True)])

    lax.fori_loop(0, 7, event, None)

    @pl.when(core == 1)
    def _():
        arrived(14)

    b0, b1 = _block(me, 7, 0), _block(me, 7, 1)
    project(14, (b0,))

    def against(new, start, stop):
        def four(i, _):
            attend([both(new, _block(me, 2 * i + j, side)) for j in (0, 1) for side in (0, 1)])

        lax.fori_loop(start, stop, four, None)

    against(b0, 0, 2)

    @pl.when(core == 0)
    def _():
        half(15, 15, 0, 17, 15, partner).wait_recv()
        half(15, 15, 0, 17, 15, partner).start()

    against(b0, 2, 3)
    attend([both(b0, _block(me, 6, 0)), both(b0, _block(me, 6, 1)), (b0, b0, True)])

    def finish(b):
        rows = pl.ds(pl.multiple_of(b * BLK, BLK), BLK)
        for n in range(N):
            at = (b * N + n) * MR
            out = mix_s[pl.ds(pl.multiple_of(at, 8), HEAD), :] * (1 / mix_s[pl.ds(pl.multiple_of(at + HEAD, 8), 1), :])
            seen_s[rows, n * HEAD : (n + 1) * HEAD] = out.astype(jnp.bfloat16).T

    def piece(dev, r, count=PIECE):
        return seen_s.at[pl.ds(pl.multiple_of(dev * ROWS + r * PIECE, PIECE), count), :]

    def part(i, theirs, c, r, count=PIECE):
        return part_s.at[i, pl.ds(pl.multiple_of(r * PIECE, PIECE), count), pl.ds(pl.multiple_of((2 * theirs + c) * W, HEAD), W)]

    def across(i, r, c, chip):
        return pltpu.make_async_remote_copy(src_ref=piece(chip + c, r), dst_ref=part(i, 1, core, r), send_sem=send2.at[17 + 8 * i + 2 * r + c],
                                            recv_sem=recv2.at[10 + 8 * i + 2 * r + core], device_id={"tp": yn + c}, device_id_type=MESH)

    def across_wait(i, r):
        for c in (0, 1):
            pltpu.make_async_remote_copy(src_ref=part(i, 1, c, r), dst_ref=part(i, 1, c, r), send_sem=send2.at[0],
                                         recv_sem=recv2.at[10 + 8 * i + 2 * r + c], device_id={"tp": partner}, device_id_type=MESH).wait_recv()

    def own(j, c):
        i, r, count = ((0, 0, BLK), (0, 2, BLK), (1, 0, ROWS))[j]
        return piece((xn, xn, base)[j] + c, r, count), part(i, 0, core, r, count)

    def hand(j):
        src, dst = own(j, 1 - core)
        return pltpu.make_async_remote_copy(src_ref=src, dst_ref=dst, send_sem=send2.at[(33, 34, 51)[j]], recv_sem=recv2.at[(26, 27, 44)[j]],
                                            device_id={"tp": partner}, device_id_type=MESH)

    def keep(j):
        src, dst = own(j, core)
        return pltpu.make_async_copy(src, dst, lsem.at[j])

    def give_own(j):
        hand(j).start()
        keep(j).start()

    def have_own(j):
        keep(j).wait()
        hand(j).wait_recv()

    def give(q, r):
        at = (pl.ds(pl.multiple_of(r * PIECE, PIECE), PIECE), pl.ds(pl.multiple_of(q * WIDE, WIDE), WIDE))
        return pltpu.make_async_remote_copy(src_ref=a_s.at[at], dst_ref=sum_s.at[at], send_sem=send2.at[35 + 4 * q + r],
                                            recv_sem=recv2.at[28 + 4 * q + r], device_id={"tp": xn + core}, device_id_type=MESH)

    def partial_sum(q, r):
        rows, columns = pl.ds(pl.multiple_of(r * PIECE, PIECE), PIECE), pl.ds(pl.multiple_of(q * WIDE, WIDE), WIDE)
        a_s[rows, columns] = _dot(part_s[0, rows, :], wo_s[:, columns], 1, 0).astype(jnp.bfloat16)
        give(q, r).start()

    def far(half):
        for c in (0, 1):
            finish(2 * (dg + c) + half)
        for r in (2 * half, 2 * half + 1):
            for c in (0, 1):
                across(0, r, c, dg).start()

    far(0)
    wo_in(0)
    wo_in(1)
    @pl.when(core == 0)
    def _():
        half(15, 15, 1, 15, 16, partner).wait_recv()
        half(15, 15, 1, 15, 16, partner).start()

    @pl.when(core == 1)
    def _():
        half(15, 15, 0, 17, 15, partner).wait_recv()
        half(15, 15, 1, 15, 16, partner).wait_recv()

    project(15, (b1,))
    attend([both(b1, _block(me, 4, 0)), both(b1, _block(me, 5, 0))])
    for c in (0, 1):
        finish(2 * (xn + c))
    give_own(0)
    attend([both(b1, _block(me, 4, 1)), both(b1, _block(me, 5, 1))])
    for i in (*range(7), *range(8, 13)):
        remote(0, 0, i, partner).wait_send()

    @pl.when(core == 0)
    def _():
        for i in (7, 13):
            remote(0, 0, i, partner).wait_send()
        for i in (14, 15, 16, 17):
            half(0, 0, 0, i, 15, partner).wait_send()

    send_wo(1 - core, 1 - core, 0, 1 - core, partner).wait_recv()
    wo_all(0)
    wo_all(1)
    have_own(0)

    def early(r, _):
        across_wait(0, r)
        partial_sum(0, r)
        partial_sum(1, r)

    lax.fori_loop(0, 1, early, None)
    against(b1, 0, 2)
    attend([both(b1, _block(me, 6, 0)), both(b1, _block(me, 6, 1)), both(b1, b0), (b1, b1, True)])
    far(1)
    wo_out(3).start()
    for c in (0, 1):
        finish(2 * (xn + c) + 1)
    give_own(1)
    lax.fori_loop(1, 2, early, None)
    for b in range(4):
        finish(2 * yn + b)
    for r in range(4):
        for c in (0, 1):
            across(1, r, c, yn).start()
    for b in range(4):
        finish(2 * base + b)
    give_own(2)
    have_own(1)
    lax.fori_loop(2, 4, early, None)
    have_own(2)

    def ours(n, _):
        out = _dot(part_s[1, :, : 2 * W], wo_s[: 2 * W, pl.ds(pl.multiple_of(n * BLK, BLK), BLK)], 1, 0)
        mix_s[pl.ds(pl.multiple_of(n * ROWS, ROWS), ROWS), :] = out

    lax.fori_loop(0, D // BLK, ours, None)
    for q in (2, 3):
        wo_in(q)
        wo_all(q)

        def late(r, _):
            partial_sum(q, r)

        lax.fori_loop(0, 4, late, None)

    def last(r, _):
        rows = pl.ds(pl.multiple_of(r * PIECE, PIECE), PIECE)
        across_wait(1, r)
        for n in range(D // BLK):
            at = pl.ds(pl.multiple_of(n * ROWS + r * PIECE, PIECE), PIECE)
            mix_s[at, :] += _dot(part_s[1, rows, 2 * W :], wo_s[2 * W :, n * BLK : (n + 1) * BLK], 1, 0)
        for q in range(4):
            give(q, r).wait_recv()
        for n in range(D // BLK):
            at = slice(n * BLK, (n + 1) * BLK)
            total = mix_s[pl.ds(pl.multiple_of(n * ROWS + r * PIECE, PIECE), PIECE), :] + sum_s[rows, at].astype(jnp.float32)
            y_ref[rows, at] = (x_ref[rows, at].astype(jnp.float32) + total).astype(jnp.bfloat16)

    lax.fori_loop(0, 4, last, None)

    send_wo(core, core, 0, core, partner).wait_send()

    for q in range(4):
        wo_out(q).wait_send()
        wo_on(q).wait_send()

    def sent(r, _):
        for c in (0, 1):
            across(0, r, c, dg).wait_send()
            across(1, r, c, yn).wait_send()
        for q in range(4):
            give(q, r).wait_send()

    lax.fori_loop(0, 4, sent, None)
    for j in range(3):
        hand(j).wait_send()


def solution(mesh):
    def step(x, gain, wq, wk, wv, wo):
        lo, hi = _rope_tables()
        any_space = pl.BlockSpec(memory_space=pl.ANY)
        vmem = pl.BlockSpec(memory_space=pltpu.VMEM)
        return pl.pallas_call(
            kernel,
            out_shape=pltpu.VMEM((ROWS, D), jnp.bfloat16),
            in_specs=[any_space, vmem, any_space, any_space, any_space, any_space, any_space, vmem],
            out_specs=vmem,
            scratch_shapes=[
                pltpu.VMEM((ROWS, D), jnp.bfloat16),
                pltpu.VMEM((2, BLK, HEAD), jnp.float32),
                pltpu.VMEM((NBLK * BLK, D), jnp.bfloat16),
                pltpu.VMEM((D, 3 * W), jnp.bfloat16),
                pltpu.VMEM((NBLK, N, BLK, HEAD), jnp.bfloat16),
                pltpu.VMEM((NBLK, N, BLK, HEAD), jnp.bfloat16),
                pltpu.VMEM((NBLK, N, VR, BLK), jnp.bfloat16),
                pltpu.VMEM((NBLK, 8, BLK), jnp.float32),
                pltpu.VMEM((NBLK * N * MR, BLK), jnp.float32),
                pltpu.VMEM((4 * W, D), jnp.bfloat16),
                pltpu.VMEM((NBLK * BLK, W), jnp.bfloat16),
                pltpu.VMEM((2, ROWS, 4 * W), jnp.bfloat16),
                pltpu.VMEM((ROWS, D), jnp.bfloat16),
                pltpu.SemaphoreType.DMA((7,)),
                pltpu.SemaphoreType.DMA((18,)),
                pltpu.SemaphoreType.DMA((17,)),
                pltpu.SemaphoreType.DMA((52,)),
                pltpu.SemaphoreType.DMA((45,)),
                pltpu.SemaphoreType.DMA((3,)),
            ],
            compiler_params=pltpu.CompilerParams(collective_id=0, has_side_effects=True, vmem_limit_bytes=61 * 2**20),
            cost_estimate=pl.CostEstimate(flops=40 * 10**9, bytes_accessed=10**7, transcendentals=3 * 10**7),
        )(x, gain, wq, wk, wv, wo, jnp.asarray(lo), jnp.asarray(hi))

    tokens, columns = P(("dp", "tp"), None), P(None, "tp")
    return jax.shard_map(
        step,
        mesh=mesh,
        in_specs=(tokens, P(None), columns, columns, columns, P("tp", None)),
        out_specs=tokens,
        check_vma=False,
    )
```

```python
import functools

import jax
import jax.numpy as jnp
import numpy as np
from jax import lax
from jax.experimental import pallas as pl
from jax.experimental.pallas import tpu as pltpu
from jax.sharding import PartitionSpec as P

MESH = pl.DeviceIdType.MESH
NEG = -1e30
HIDDEN = 2 * NEG
LOG2E = 1.4426950408889634
HEAD = 128
THETA = 10000
WIDE = 512
PIECE = 128
AHEAD = 6
N = 3
BLK = 256
ROWS = 512
NBLK = 16
D = 2048
W = N * HEAD
VR = 144
MR = HEAD + 8


def _dot(a, b, ca, cb):
    return lax.dot_general(a, b, (((ca,), (cb,)), ((), ())), preferred_element_type=jnp.float32)


def _rope_tables():
    half = HEAD // 2
    freq = THETA ** (-np.arange(half, dtype=np.float64) / half)
    sign = np.concatenate([-np.ones(half), np.ones(half)])
    def table(pos):
        ang = pos[:, None] * np.concatenate([freq, freq])
        return np.cos(ang).astype(np.float32), (np.sin(ang) * sign).astype(np.float32)
    lo = np.stack(table(np.arange(BLK, dtype=np.float64)))
    hi = np.stack(table(np.arange(NBLK, dtype=np.float64) * BLK))
    return lo, hi


def _place(me):
    core = me % 2
    y = (me // 2) % 2
    x = me // 4
    base = me - core
    xn = base + 4 - 8 * x
    yn = base + 2 - 4 * y
    dg = xn + 2 - 4 * y
    return core, base, xn, yn, dg


def _block(me, k, side):
    core, base, xn, yn, dg = _place(me)
    odd = k % 2
    flip = side + odd - 2 * side * odd
    near = jnp.where(side == 0, xn, yn) if not isinstance(side, int) else (xn if side == 0 else yn)
    dev = jnp.where(k < 1, me, jnp.where(k < 2, me + 1 - 2 * core, jnp.where(k < 6, near + flip, dg + 1 - flip)))
    half = jnp.where((k == 2) | (k == 3), 1 - side, side)
    return 2 * dev + half


def kernel(x_hbm, gain_ref, wq_ref, wk_ref, wv_ref, wo_ref, lo_hbm, hi_ref, y_ref,
           x_ref, lo_ref, a_s, w_s, q_s, k_s, v_s, top_s, mix_s, wo_s, seen_s, part_s, sum_s, wsem, send, recv, send2, recv2, lsem):
    me = lax.axis_index("tp")
    core, base, xn, yn, dg = _place(me)
    partner = base + 1 - core
    link = jnp.where(core == 0, xn, yn + 1)
    first = 1 - core

    def fetch(half, sem):
        rows = pl.ds(pl.multiple_of(half * BLK, BLK), BLK)
        return pltpu.make_async_copy(x_hbm.at[rows, :], x_ref.at[rows, :], wsem.at[sem])

    fetch(first, 4).start()
    fetch(1 - first, 5).start()

    barrier = pltpu.get_barrier_semaphore()
    for other in (partner, xn + core, yn, yn + 1):
        pl.semaphore_signal(barrier, inc=1, device_id={"tp": other}, device_id_type=MESH)

    loads = [pltpu.make_async_copy(w, w_s.at[:, pl.ds(i * W, W)], wsem.at[i]) for i, w in enumerate((wq_ref, wk_ref, wv_ref))]
    loads.append(pltpu.make_async_copy(lo_hbm, lo_ref, wsem.at[6]))
    for c in loads:
        c.start()
    wo_mine = wo_s.at[pl.ds(pl.multiple_of(core * W, W), W), :]
    wo_load = pltpu.make_async_copy(wo_ref, wo_mine, wsem.at[3])
    wo_load.start()

    def slot(s):
        return a_s.at[pl.ds(pl.multiple_of(s * BLK, BLK), BLK), :]

    def remote(src, dst, sem, dev):
        return pltpu.make_async_remote_copy(src_ref=slot(src), dst_ref=slot(dst), send_sem=send.at[sem], recv_sem=recv.at[dst],
                                            device_id={"tp": dev}, device_id_type=MESH)

    def send_wo(src, dst, sem, arrival, dev, q=None):
        columns = slice(None) if q is None else pl.ds(pl.multiple_of(q * WIDE, WIDE), WIDE)
        at = lambda i: wo_s.at[pl.ds(pl.multiple_of(i * W, W), W), columns]
        return pltpu.make_async_remote_copy(src_ref=at(src), dst_ref=at(dst), send_sem=send2.at[sem], recv_sem=recv2.at[arrival],
                                            device_id={"tp": dev}, device_id_type=MESH)

    def wo_out(q):
        return send_wo(core, 2 + core, 1 + q, 2 + 2 * q + core, yn + core, q)

    def wo_on(q):
        return send_wo(2 + core, 2 + core, 5 + q, 2 + 2 * q + core, partner, q)

    def wo_in(q):
        send_wo(2 + core, 2 + core, 0, 2 + 2 * q + core, partner, q).wait_recv()
        wo_on(q).start()

    def wo_all(q):
        send_wo(3 - core, 3 - core, 0, 3 + 2 * q - core, partner, q).wait_recv()

    def half(src, dst, h, sem, arrival, dev):
        at = lambda i: a_s.at[pl.ds(pl.multiple_of(i * BLK + h * PIECE, PIECE), PIECE), :]
        return pltpu.make_async_remote_copy(src_ref=at(src), dst_ref=at(dst), send_sem=send.at[sem], recv_sem=recv.at[arrival],
                                            device_id={"tp": dev}, device_id_type=MESH)

    def arrived(s):
        return pltpu.make_async_remote_copy(src_ref=slot(s), dst_ref=slot(s), send_sem=send.at[0], recv_sem=recv.at[s],
                                            device_id={"tp": partner}, device_id_type=MESH).wait_recv()

    gain = gain_ref[...].astype(jnp.float32).reshape(1, D)

    def norm(start, count):
        def rows(i, _):
            at = pl.ds(pl.multiple_of(start + i * 16, 16), 16)
            wide = x_ref[at, :].astype(jnp.float32)
            scale = lax.rsqrt(jnp.mean(wide * wide, -1, keepdims=True) + 1e-6)
            a_s[at, :] = (wide * scale * gain).astype(jnp.bfloat16)
        lax.fori_loop(0, count // 16, rows, None, unroll=8 if count == 256 else 2)

    fetch(first, 4).wait()
    norm(first * BLK, BLK)
    fetch(1 - first, 5).wait()
    pl.semaphore_wait(barrier, 4)
    norm((1 - first) * BLK, 32)
    remote(first, 4 + core, 2, link).start()
    remote(first, 2 + first, 0, partner).start()
    norm((1 - first) * BLK + 32, BLK - 32)
    v_s[:, :, HEAD:, :] = jnp.ones((NBLK, N, VR - HEAD, BLK), jnp.bfloat16)
    top_s[...] = jnp.full(top_s.shape, NEG, jnp.float32)

    def clear(i, _):
        mix_s[pl.ds(pl.multiple_of(i * MR, MR), MR), :] = jnp.zeros((MR, BLK), jnp.float32)

    lax.fori_loop(0, NBLK * N, clear, None)
    remote(1 - first, 3 - first, 1, partner).start()
    for c in loads:
        c.wait()
    wo_load.wait()
    send_wo(core, core, 0, core, partner).start()

    scale_e = HEAD ** -0.5 * LOG2E

    def project(first_slot, blocks):
        here = pl.ds(pl.multiple_of(first_slot * BLK, BLK), BLK * len(blocks))
        tables = []
        for b in blocks:
            ch, sh = hi_ref[0, pl.ds(b, 1), :], hi_ref[1, pl.ds(b, 1), :]
            cl, sl = lo_ref[0], lo_ref[1]
            tables.append((ch * cl - sh * sl, sh * cl + ch * sl))
        for g in range(0, 3 * N, 2):
            width = min(2, 3 * N - g) * HEAD
            out = _dot(a_s[here, :], w_s[:, g * HEAD : g * HEAD + width], 1, 0).astype(jnp.bfloat16)
            for i in range(width // HEAD):
                kind, n = divmod(g + i, N)
                for b, block in enumerate(blocks):
                    t = out[b * BLK : (b + 1) * BLK, i * HEAD : (i + 1) * HEAD]
                    if kind == 2:
                        v_s[block, n, :HEAD, :] = t.T
                    else:
                        t = t.astype(jnp.float32)
                        t = t * tables[b][0] + pltpu.roll(t, HEAD // 2, 1) * tables[b][1]
                        (q_s if kind == 0 else k_s)[block, n] = t.astype(jnp.bfloat16)

    def attend(pairs):
        strips = [(q, k, masked, n) for q, k, masked in pairs for n in range(N)]
        if any(masked for _, _, masked in pairs):
            ok = lax.broadcasted_iota(jnp.int32, (BLK, BLK), 1) >= lax.broadcasted_iota(jnp.int32, (BLK, BLK), 0)

        def score(q, k, masked, n):
            return _dot(k_s[k, n], q_s[q, n], 1, 1)

        ahead = [score(*strip) for strip in strips[:AHEAD]]
        for i, (q, k, masked, n) in enumerate(strips):
            if i + AHEAD < len(strips):
                ahead.append(score(*strips[i + AHEAD]))
            s = ahead.pop(0)
            if masked:
                s = jnp.where(ok, s, HIDDEN)
            old = top_s[q, n : n + 1, :]
            top = jnp.maximum(old, s.max(axis=0, keepdims=True))
            top_s[q, n : n + 1, :] = top
            p = jnp.exp2((s - top) * scale_e).astype(jnp.bfloat16)
            keep = jnp.exp2((old - top) * scale_e)
            mix = pl.ds(pl.multiple_of((q * N + n) * MR, 8), MR)
            mix_s[mix, :] = mix_s[mix, :] * keep + _dot(v_s[k, n], p, 1, 0)[:MR, :]

    def both(new, old):
        return jnp.maximum(new, old), jnp.minimum(new, old), False

    def event(k, _):
        b0, b1 = _block(me, k, 0), _block(me, k, 1)

        @pl.when(k >= 2)
        def _():
            arrived(2 * k + 1 - core)

            @pl.when((k == 2) | ((k == 3) & (core == 0)))
            def _():
                remote(2 * k + 1 - core, 2 * k + 8 + core, 4 + k, link).start()

            @pl.when((k == 4) & (core == 0))
            def _():
                half(9, 15, 0, 16, 15, link).start()
                half(9, 15, 1, 14, 16, link).start()

            @pl.when((k == 3) & (core == 1))
            def _():
                wo_out(0).start()
                wo_out(1).start()
                wo_out(2).start()

        project(2 * k, (b0, b1))

        @pl.when(k == 0)
        def _():
            arrived(2 + first)
            remote(2 + first, 6 + core, 3, link).start()
            remote(1 - first, 8 + core, 4, link).start()
            arrived(3 - first)
            remote(3 - first, 10 + core, 5, link).start()

        def older(j, _):
            pairs = []
            for new in (b0, b1):
                for side in (0, 1):
                    pairs.append(both(new, _block(me, j, side)))
            attend(pairs)

        @pl.when((k == 6) & (core == 0))
        def _():
            wo_out(0).start()
            wo_out(1).start()
            wo_out(2).start()

        lax.fori_loop(0, k, older, None)

        @pl.when((k >= 1) & ((k < 6) | (core == 0)))
        def _():
            arrived(2 * k + 2 + core)
            remote(2 * k + 2 + core, 2 * k + 2 + core, 7 + k, partner).start()


        attend([both(b0, b1), (b0, b0, True), (b1, b1, True)])

    lax.fori_loop(0, 7, event, None)

    @pl.when(core == 1)
    def _():
        arrived(14)

    b0, b1 = _block(me, 7, 0), _block(me, 7, 1)
    project(14, (b0,))

    def against(new, start, stop):
        def four(i, _):
            attend([both(new, _block(me, 2 * i + j, side)) for j in (0, 1) for side in (0, 1)])

        lax.fori_loop(start, stop, four, None, unroll=True)

    against(b0, 0, 2)

    @pl.when(core == 0)
    def _():
        half(15, 15, 0, 17, 15, partner).wait_recv()
        half(15, 15, 0, 17, 15, partner).start()

    against(b0, 2, 3)
    attend([both(b0, _block(me, 6, 0)), both(b0, _block(me, 6, 1)), (b0, b0, True)])

    def finish(b):
        rows = pl.ds(pl.multiple_of(b * BLK, BLK), BLK)
        for n in range(N):
            at = (b * N + n) * MR
            out = mix_s[pl.ds(pl.multiple_of(at, 8), HEAD), :] * (1 / mix_s[pl.ds(pl.multiple_of(at + HEAD, 8), 1), :])
            seen_s[rows, n * HEAD : (n + 1) * HEAD] = out.astype(jnp.bfloat16).T

    def piece(dev, r, count=PIECE):
        return seen_s.at[pl.ds(pl.multiple_of(dev * ROWS + r * PIECE, PIECE), count), :]

    def part(i, theirs, c, r, count=PIECE):
        return part_s.at[i, pl.ds(pl.multiple_of(r * PIECE, PIECE), count), pl.ds(pl.multiple_of((2 * theirs + c) * W, HEAD), W)]

    def across(i, r, c, chip):
        return pltpu.make_async_remote_copy(src_ref=piece(chip + c, r), dst_ref=part(i, 1, core, r), send_sem=send2.at[17 + 8 * i + 2 * r + c],
                                            recv_sem=recv2.at[10 + 8 * i + 2 * r + core], device_id={"tp": yn + c}, device_id_type=MESH)

    def across_wait(i, r):
        for c in (0, 1):
            pltpu.make_async_remote_copy(src_ref=part(i, 1, c, r), dst_ref=part(i, 1, c, r), send_sem=send2.at[0],
                                         recv_sem=recv2.at[10 + 8 * i + 2 * r + c], device_id={"tp": partner}, device_id_type=MESH).wait_recv()

    def own(j, c):
        i, r, count = ((0, 0, BLK), (0, 2, BLK), (1, 0, ROWS))[j]
        return piece((xn, xn, base)[j] + c, r, count), part(i, 0, core, r, count)

    def hand(j):
        src, dst = own(j, 1 - core)
        return pltpu.make_async_remote_copy(src_ref=src, dst_ref=dst, send_sem=send2.at[(33, 34, 51)[j]], recv_sem=recv2.at[(26, 27, 44)[j]],
                                            device_id={"tp": partner}, device_id_type=MESH)

    def keep(j):
        src, dst = own(j, core)
        return pltpu.make_async_copy(src, dst, lsem.at[j])

    def give_own(j):
        hand(j).start()
        keep(j).start()

    def have_own(j):
        keep(j).wait()
        hand(j).wait_recv()

    def give(q, r):
        at = (pl.ds(pl.multiple_of(r * PIECE, PIECE), PIECE), pl.ds(pl.multiple_of(q * WIDE, WIDE), WIDE))
        return pltpu.make_async_remote_copy(src_ref=a_s.at[at], dst_ref=sum_s.at[at], send_sem=send2.at[35 + 4 * q + r],
                                            recv_sem=recv2.at[28 + 4 * q + r], device_id={"tp": xn + core}, device_id_type=MESH)

    def partial_sum(q, r):
        rows, columns = pl.ds(pl.multiple_of(r * PIECE, PIECE), PIECE), pl.ds(pl.multiple_of(q * WIDE, WIDE), WIDE)
        a_s[rows, columns] = _dot(part_s[0, rows, :], wo_s[:, columns], 1, 0).astype(jnp.bfloat16)
        give(q, r).start()

    def far(half):
        for c in (0, 1):
            finish(2 * (dg + c) + half)
        for r in (2 * half, 2 * half + 1):
            for c in (0, 1):
                across(0, r, c, dg).start()

    far(0)
    wo_in(0)
    wo_in(1)
    @pl.when(core == 0)
    def _():
        half(15, 15, 1, 15, 16, partner).wait_recv()
        half(15, 15, 1, 15, 16, partner).start()

    @pl.when(core == 1)
    def _():
        half(15, 15, 0, 17, 15, partner).wait_recv()
        half(15, 15, 1, 15, 16, partner).wait_recv()

    project(15, (b1,))
    attend([both(b1, _block(me, 4, 0)), both(b1, _block(me, 5, 0))])
    for c in (0, 1):
        finish(2 * (xn + c))
    give_own(0)
    attend([both(b1, _block(me, 4, 1)), both(b1, _block(me, 5, 1))])
    for i in (*range(7), *range(8, 13)):
        remote(0, 0, i, partner).wait_send()

    @pl.when(core == 0)
    def _():
        for i in (7, 13):
            remote(0, 0, i, partner).wait_send()
        for i in (14, 15, 16, 17):
            half(0, 0, 0, i, 15, partner).wait_send()

    send_wo(1 - core, 1 - core, 0, 1 - core, partner).wait_recv()
    wo_all(0)
    wo_all(1)
    have_own(0)

    def early(r, _):
        across_wait(0, r)
        partial_sum(0, r)
        partial_sum(1, r)

    lax.fori_loop(0, 1, early, None)
    against(b1, 0, 2)
    attend([both(b1, _block(me, 6, 0)), both(b1, _block(me, 6, 1)), both(b1, b0), (b1, b1, True)])
    far(1)
    wo_out(3).start()
    for c in (0, 1):
        finish(2 * (xn + c) + 1)
    give_own(1)
    lax.fori_loop(1, 2, early, None)
    for b in range(4):
        finish(2 * yn + b)
    for r in range(4):
        for c in (0, 1):
            across(1, r, c, yn).start()
    for b in range(4):
        finish(2 * base + b)
    give_own(2)
    have_own(1)
    lax.fori_loop(2, 4, early, None)
    have_own(2)

    def ours(n, _):
        out = _dot(part_s[1, :, : 2 * W], wo_s[: 2 * W, pl.ds(pl.multiple_of(n * BLK, BLK), BLK)], 1, 0)
        mix_s[pl.ds(pl.multiple_of(n * ROWS, ROWS), ROWS), :] = out

    lax.fori_loop(0, D // BLK, ours, None)
    for q in (2, 3):
        wo_in(q)
        wo_all(q)

        def late(r, _):
            partial_sum(q, r)

        lax.fori_loop(0, 4, late, None)

    def last(r, _):
        rows = pl.ds(pl.multiple_of(r * PIECE, PIECE), PIECE)
        across_wait(1, r)
        for n in range(D // BLK):
            at = pl.ds(pl.multiple_of(n * ROWS + r * PIECE, PIECE), PIECE)
            mix_s[at, :] += _dot(part_s[1, rows, 2 * W :], wo_s[2 * W :, n * BLK : (n + 1) * BLK], 1, 0)
        for q in range(4):
            give(q, r).wait_recv()
        for n in range(D // BLK):
            at = slice(n * BLK, (n + 1) * BLK)
            total = mix_s[pl.ds(pl.multiple_of(n * ROWS + r * PIECE, PIECE), PIECE), :] + sum_s[rows, at].astype(jnp.float32)
            y_ref[rows, at] = (x_ref[rows, at].astype(jnp.float32) + total).astype(jnp.bfloat16)

    lax.fori_loop(0, 4, last, None)

    send_wo(core, core, 0, core, partner).wait_send()

    for q in range(4):
        wo_out(q).wait_send()
        wo_on(q).wait_send()

    def sent(r, _):
        for c in (0, 1):
            across(0, r, c, dg).wait_send()
            across(1, r, c, yn).wait_send()
        for q in range(4):
            give(q, r).wait_send()

    lax.fori_loop(0, 4, sent, None)
    for j in range(3):
        hand(j).wait_send()


def solution(mesh):
    def step(x, gain, wq, wk, wv, wo):
        lo, hi = _rope_tables()
        any_space = pl.BlockSpec(memory_space=pl.ANY)
        vmem = pl.BlockSpec(memory_space=pltpu.VMEM)
        return pl.pallas_call(
            kernel,
            out_shape=pltpu.VMEM((ROWS, D), jnp.bfloat16),
            in_specs=[any_space, vmem, any_space, any_space, any_space, any_space, any_space, vmem],
            out_specs=vmem,
            scratch_shapes=[
                pltpu.VMEM((ROWS, D), jnp.bfloat16),
                pltpu.VMEM((2, BLK, HEAD), jnp.float32),
                pltpu.VMEM((NBLK * BLK, D), jnp.bfloat16),
                pltpu.VMEM((D, 3 * W), jnp.bfloat16),
                pltpu.VMEM((NBLK, N, BLK, HEAD), jnp.bfloat16),
                pltpu.VMEM((NBLK, N, BLK, HEAD), jnp.bfloat16),
                pltpu.VMEM((NBLK, N, VR, BLK), jnp.bfloat16),
                pltpu.VMEM((NBLK, 8, BLK), jnp.float32),
                pltpu.VMEM((NBLK * N * MR, BLK), jnp.float32),
                pltpu.VMEM((4 * W, D), jnp.bfloat16),
                pltpu.VMEM((NBLK * BLK, W), jnp.bfloat16),
                pltpu.VMEM((2, ROWS, 4 * W), jnp.bfloat16),
                pltpu.VMEM((ROWS, D), jnp.bfloat16),
                pltpu.SemaphoreType.DMA((7,)),
                pltpu.SemaphoreType.DMA((18,)),
                pltpu.SemaphoreType.DMA((17,)),
                pltpu.SemaphoreType.DMA((52,)),
                pltpu.SemaphoreType.DMA((45,)),
                pltpu.SemaphoreType.DMA((3,)),
            ],
            compiler_params=pltpu.CompilerParams(collective_id=0, has_side_effects=True, vmem_limit_bytes=61 * 2**20),
            cost_estimate=pl.CostEstimate(flops=40 * 10**9, bytes_accessed=10**7, transcendentals=3 * 10**7),
        )(x, gain, wq, wk, wv, wo, jnp.asarray(lo), jnp.asarray(hi))

    tokens, columns = P(("dp", "tp"), None), P(None, "tp")
    return jax.shard_map(
        step,
        mesh=mesh,
        in_specs=(tokens, P(None), columns, columns, columns, P("tp", None)),
        out_specs=tokens,
        check_vma=False,
    )
```
